256 devices in a mesh: seq: 32 (over z, y), tp: 8 (over x, core).
Axes of the slice: x: 4, y: 4, z: 8, core: 2. Of those that a mesh axis runs over, the one named last changes fastest.
Arguments:
- query_act: bfloat16 [8192, 4096], P('seq', 'tp'), may hold values from -6 to 6
- key_act: bfloat16 [8192, 1024], P('seq', 'tp'), may hold values from -6 to 6
- value_act: bfloat16 [8192, 1024], P('seq', 'tp'), may hold values from -6 to 6
- attn_out: bfloat16 [8192, 4096], P('seq', 'tp'), may hold values from -6 to 6
- out_grad: bfloat16 [8192, 4096], P('seq', 'tp'), may hold values from -6 to 6
- log_sum: float32 [32, 8192], P('tp', 'seq'), as said below
- positions: int32 [8192], P('seq'), may hold values from 0 to 8191, as said below
- w_query: bfloat16 [4096, 4096], P(None, 'tp'), may hold values from -0.09375 to 0.09375
- w_key: bfloat16 [4096, 1024], P(None, 'tp'), may hold values from -0.09375 to 0.09375
- w_value: bfloat16 [4096, 1024], P(None, 'tp'), may hold values from -0.09375 to 0.09375
Outputs:
- input_grad: bfloat16 [8192, 4096], P('seq', 'tp')
The draws below stay inside these ranges and needn't reach their ends.
Inputs may be any that keep to these rules, and one draw needn't show every extreme that they name: The rows of one index of seq are two runs of 128 consecutive positions, each run starting at a multiple of 128; all rows together hold every position 0 to 8191 once. log_sum[h, t] lies within 0.5 of log(positions[t] + 1) + 0.5.
All inputs are finite; a program needn't handle non-finite values.
Results may differ from the reference program's by a relative error of at most 0.0057.
Values may be sent and summed in bfloat16 or wider, within the bound.
No kernel may reach another device: no remote copies, remote signals or barrier semaphores. Data moves between devices by JAX's collectives and lax.ppermute only.
A program may use at most 64 MiB of HBM per device.

```python
import jax
import jax.numpy as jnp
from jax import lax

D = 4096
HEADS = 32
KV_HEADS = 8
HEAD_DIM = 128
TOK_DEV = 256
TOKENS = 8192


def shared_places(key):
    count = 2 * (TOKENS // TOK_DEV)
    half_rows = TOK_DEV // 2
    order = jax.random.permutation(jax.random.fold_in(key, 71), count)
    return (order[:, None] * half_rows + jnp.arange(half_rows)[None, :]).reshape(-1).astype(jnp.int32)


def draw_positions(key, part):
    return shared_places(key)


def draw_log_sum(key, part):
    places = shared_places(key).astype(jnp.float32)
    noise = jax.random.uniform(jax.random.fold_in(key, 23), (HEADS, TOKENS), jnp.float32, -0.25, 0.25)
    return jnp.log(places + 1.0)[None, :] + 0.5 + noise


def block_scale(rng, dims, split, least, top_value):
    gain, own = 1.0, jax.random.fold_in(rng, 6)
    for axis_at, blocks in split:
        draws = jnp.exp(jax.random.uniform(jax.random.fold_in(own, axis_at), (blocks,), jnp.float32, least / len(split), top_value / len(split)))
        gain = gain * jnp.repeat(draws, dims[axis_at] // blocks).reshape([-1 if axis == axis_at else 1 for axis in range(len(dims))])
    return gain


def scatter_about(key, extent, width, bound, split=(), held_as=jnp.bfloat16):
    entries = jax.random.normal(key, extent, jnp.float32) * width
    if len(split) > 0:
        entries = block_scale(key, extent, split, -0.22, 0.18) * entries
    return jnp.clip(entries, min=-bound, max=bound).astype(held_as)


def setup_inputs(seed: int = 0) -> dict:
    key_list = jax.random.split(jax.random.key(seed), 11)
    query_act = scatter_about(key_list[0], (TOKENS, HEADS * HEAD_DIM), 1.0, 6.0, ((0, 32), (1, 8)))
    key_act = scatter_about(key_list[1], (TOKENS, KV_HEADS * HEAD_DIM), 1.0, 6.0, ((0, 32), (1, 8)))
    value_act = scatter_about(key_list[2], (TOKENS, KV_HEADS * HEAD_DIM), 1.0, 6.0, ((0, 32), (1, 8)))
    attn_out = scatter_about(key_list[3], (TOKENS, HEADS * HEAD_DIM), 0.5, 6.0, ((0, 32), (1, 8)))
    out_grad = scatter_about(key_list[4], (TOKENS, HEADS * HEAD_DIM), 1.0, 6.0, ((0, 32), (1, 8)))
    log_sum = draw_log_sum(jax.random.fold_in(key_list[10], 71), 0)
    positions = draw_positions(jax.random.fold_in(key_list[10], 71), 0)
    w_query = scatter_about(key_list[7], (D, HEADS * HEAD_DIM), D ** -0.5, 0.09375, ((1, 8),))
    w_key = scatter_about(key_list[8], (D, KV_HEADS * HEAD_DIM), D ** -0.5, 0.09375, ((1, 8),))
    w_value = scatter_about(key_list[9], (D, KV_HEADS * HEAD_DIM), D ** -0.5, 0.09375, ((1, 8),))
    return {"query_act": query_act, "key_act": key_act, "value_act": value_act, "attn_out": attn_out, "out_grad": out_grad, "log_sum": log_sum, "positions": positions, "w_query": w_query, "w_key": w_key, "w_value": w_value}


def rotate_back(grads, places):
    half_dim = grads.shape[-1] // 2
    freqs = 500000.0 ** (-(jnp.arange(half_dim, dtype=jnp.float32) * 2.0 / grads.shape[-1]))
    angles = places.astype(jnp.float32)[:, None] * freqs[None, :]
    cosine = jnp.cos(angles)[:, None, :]
    sine = jnp.sin(angles)[:, None, :]
    first = grads[..., :half_dim]
    second = grads[..., half_dim:]
    return jnp.concatenate([first * cosine + second * sine, second * cosine - first * sine], axis=-1)


def reference(query_act, key_act, value_act, attn_out, out_grad, log_sum, positions, w_query, w_key, w_value):
    tokens = query_act.shape[0]
    repeat = HEADS // KV_HEADS
    scale = HEAD_DIM ** -0.5
    query_heads = query_act.reshape(tokens, KV_HEADS, repeat, HEAD_DIM).transpose(1, 0, 2, 3)
    dout_heads = out_grad.reshape(tokens, KV_HEADS, repeat, HEAD_DIM).transpose(1, 0, 2, 3)
    output_heads = attn_out.reshape(tokens, KV_HEADS, repeat, HEAD_DIM).transpose(1, 0, 2, 3)
    deltas = jnp.sum(dout_heads.astype(jnp.float32) * output_heads.astype(jnp.float32), -1)
    lse_heads = log_sum.reshape(KV_HEADS, repeat, tokens)
    key_heads = key_act.reshape(tokens, KV_HEADS, HEAD_DIM).transpose(1, 0, 2)
    value_heads = value_act.reshape(tokens, KV_HEADS, HEAD_DIM).transpose(1, 0, 2)
    blocks = tokens // TOK_DEV

    def one_group(operands):
        query_group, dout_group, delta_group, lse_group, key_group, value_group = operands
        query_float = query_group.astype(jnp.float32)
        dout_float = dout_group.astype(jnp.float32)

        def one_block(dq_total, block_index):
            start = (block_index * TOK_DEV).astype(jnp.int32)
            key_block = lax.dynamic_slice_in_dim(key_group, start, TOK_DEV, 0).astype(jnp.float32)
            value_block = lax.dynamic_slice_in_dim(value_group, start, TOK_DEV, 0).astype(jnp.float32)
            key_places = lax.dynamic_slice_in_dim(positions, start, TOK_DEV, 0)
            scores = jnp.einsum('qrd,kd->rqk', query_float, key_block) * scale
            visible = key_places[None, :] <= positions[:, None]
            probs = jnp.where(visible[None], jnp.exp(scores - lse_group[:, :, None]), 0.0)
            probs_low = lax.optimization_barrier(probs.astype(jnp.bfloat16)).astype(jnp.float32)
            value_grad = jnp.einsum('rqk,qrd->kd', probs_low, dout_float)
            prob_grad = jnp.einsum('qrd,kd->rqk', dout_float, value_block)
            score_grad = probs * (prob_grad - delta_group.T[:, :, None]) * scale
            score_low = lax.optimization_barrier(score_grad.astype(jnp.bfloat16)).astype(jnp.float32)
            dq_total = dq_total + jnp.einsum('rqk,kd->qrd', score_low, key_block)
            key_grad = jnp.einsum('rqk,qrd->kd', score_low, query_float)
            return dq_total, (key_grad, value_grad)

        start_dq = jnp.zeros((tokens, repeat, HEAD_DIM), jnp.float32)
        dq_total, (key_parts, value_parts) = lax.scan(one_block, start_dq, jnp.arange(blocks, dtype=jnp.int32))
        return dq_total, key_parts.reshape(tokens, HEAD_DIM), value_parts.reshape(tokens, HEAD_DIM)

    dq_all, dk_all, dv_all = lax.map(one_group, (query_heads, dout_heads, deltas, lse_heads, key_heads, value_heads))
    dq_all = dq_all.transpose(1, 0, 2, 3).reshape(tokens, HEADS, HEAD_DIM)
    dk_all = dk_all.transpose(1, 0, 2)
    dv_all = dv_all.transpose(1, 0, 2)
    query_grad = rotate_back(dq_all, positions).reshape(tokens, HEADS * HEAD_DIM).astype(jnp.bfloat16)
    key_grad = rotate_back(dk_all, positions).reshape(tokens, KV_HEADS * HEAD_DIM).astype(jnp.bfloat16)
    value_grad = dv_all.reshape(tokens, KV_HEADS * HEAD_DIM).astype(jnp.bfloat16)
    total = jnp.dot(query_grad, w_query.T, preferred_element_type=jnp.float32)
    total = total + jnp.dot(key_grad, w_key.T, preferred_element_type=jnp.float32)
    total = total + jnp.dot(value_grad, w_value.T, preferred_element_type=jnp.float32)
    return total.astype(jnp.bfloat16)
```

```python
import functools

import jax
import jax.numpy as jnp
from jax import lax
from jax.experimental import pallas as pl
from jax.experimental.pallas import tpu as pltpu
from jax.sharding import PartitionSpec as P

HEADS = 32
KV_HEADS = 8
HEAD_DIM = 128
REPEAT = HEADS // KV_HEADS
HALF = HEAD_DIM // 2
CHUNK = 128
ROWS = 256
NZ, NY, NX, NC = 8, 4, 4, 2
LOG2E = 1.4426950408889634
SCALE = HEAD_DIM**-0.5
BF = jnp.bfloat16
F32 = jnp.float32
PIECE = CHUNK + 16
UNROLL = 2


def dot(a, b, dims, precision=None):
    return lax.dot_general(
        a, b, (dims, ((), ())), preferred_element_type=F32, precision=precision
    )


NN = ((1,), (0,))
NT = ((1,), (1,))


def move_z(value, steps):
    pairs = [
        (z * NY + y, ((z + steps) % NZ) * NY + y) for z in range(NZ) for y in range(NY)
    ]
    return lax.ppermute(value, "seq", pairs)


def move_y(value, steps):
    pairs = [
        (z * NY + y, z * NY + (y + steps) % NY) for z in range(NZ) for y in range(NY)
    ]
    return lax.ppermute(value, "seq", pairs)


def move_x(value, steps):
    pairs = [
        (x * NC + c, ((x + steps) % NX) * NC + c) for x in range(NX) for c in range(NC)
    ]
    return lax.ppermute(value, "tp", pairs)


def swap_core(value):
    pairs = [(x * NC + c, x * NC + 1 - c) for x in range(NX) for c in range(NC)]
    return lax.ppermute(value, "tp", pairs)


def split3(value):
    high = value.astype(BF)
    rest = value - high.astype(F32)
    mid = rest.astype(BF)
    low = (rest - mid.astype(F32)).astype(BF)
    return high, mid, low


def prep_kernel(pos_ref, q_ref, do_ref, o_ref, lse_ref, k_ref, v_ref, pack_ref, kv_ref):
    ones = jnp.ones((8, HEAD_DIM), F32)
    deltas = []
    for head in range(REPEAT):
        lanes = slice(head * 128, head * 128 + 128)
        prod = do_ref[:, lanes].astype(F32) * o_ref[:, lanes].astype(F32)
        deltas.append(dot(ones, prod, NT, lax.Precision.HIGHEST)[0:1])
    kv_ref[0:ROWS, 0:128] = k_ref[...]
    kv_ref[0:ROWS, 128:256] = v_ref[...]
    index = lax.broadcasted_iota(jnp.int32, (16, 256), 0)
    first = (pos_ref[0] // CHUNK).astype(F32)
    second = (pos_ref[CHUNK] // CHUNK).astype(F32)
    kv_ref[ROWS : ROWS + 16, :] = jnp.where(index == 0, first, second).astype(BF)
    for c in range(2):
        base = c * PIECE
        rows = slice(c * CHUNK, c * CHUNK + CHUNK)
        pack_ref[base : base + CHUNK, 0:512] = q_ref[rows, :]
        pack_ref[base : base + CHUNK, 512:1024] = do_ref[rows, :]
        lse_row = jnp.concatenate([lse_ref[h : h + 1, rows] for h in range(REPEAT)], axis=1)
        delta_row = jnp.concatenate([deltas[h][:, rows] for h in range(REPEAT)], axis=1)
        row = jnp.concatenate([lse_row * LOG2E, delta_row * SCALE], axis=1)
        parts = [part.astype(F32) for part in split3(row)]
        parts.append(jnp.full((1, 1024), second if c else first, F32))
        block = jnp.concatenate(parts + [jnp.zeros((12, 1024), F32)], axis=0)
        pack_ref[base + CHUNK : base + PIECE, :] = block.astype(BF)


def attn_kernel(q_sizes, nkv, has_dq, has_dkv, *refs):
    refs = list(refs)

    def take(count):
        out = refs[:count]
        del refs[:count]
        return out

    packs = take(len(q_sizes))
    kvs = take(nkv)
    dq_ins = take(sum(has_dq))
    dkv_ins = take(sum(has_dkv))
    nblocks = sum(q_sizes) // 2
    dq_outs = take(nblocks)
    dkv_outs = take(nkv)
    qc, doc, ks, vs, kts, rowc, dq_acc, dk_acc, dv_acc, qst, kst, ln, l1, l2, lt1, lt2 = refs
    nq = 2 * nblocks
    nk = 2 * nkv

    n = 0
    for ref, size in zip(packs, q_sizes):
        for c in range(size):
            base = c * PIECE
            meta = ref[base + CHUNK : base + PIECE, :].astype(F32)
            row = meta[0:1] + meta[1:2] + meta[2:3]
            rowc[n] = jnp.broadcast_to(row, (8, 1024))
            qst[n] = jnp.max(meta[3:4, 0:128]).astype(jnp.int32)
            for h in range(REPEAT):
                rows = slice(h * 128, h * 128 + 128)
                qc[n, rows, :] = ref[base : base + CHUNK, h * 128 : h * 128 + 128]
                doc[n, rows, :] = ref[base : base + CHUNK, 512 + h * 128 : 640 + h * 128]
            n += 1
    for j in range(nkv):
        meta = kvs[j][ROWS : ROWS + 16, :].astype(F32)
        for c in range(2):
            rows = slice(c * 128, c * 128 + 128)
            kst[2 * j + c] = jnp.max(meta[c : c + 1, 0:128]).astype(jnp.int32)
            ks[2 * j + c] = kvs[j][rows, 0:128]
            vs[2 * j + c] = kvs[j][rows, 128:256]
            kts[2 * j + c] = kvs[j][rows, 0:128].T
    at = 0
    for b in range(nblocks):
        for c in range(2):
            for h in range(REPEAT):
                lanes = slice(h * 128, h * 128 + 128)
                if has_dq[b]:
                    dq_acc[2 * b + c, :, lanes] = dq_ins[at][lanes, c * 128 : c * 128 + 128]
                else:
                    dq_acc[2 * b + c, :, lanes] = jnp.zeros((128, 128), F32)
        at += has_dq[b]
    at = 0
    for j in range(nkv):
        for c in range(2):
            rows = slice(c * 128, c * 128 + 128)
            if has_dkv[j]:
                dk_acc[2 * j + c] = dkv_ins[at][rows, 0:128]
                dv_acc[2 * j + c] = dkv_ins[at][rows, 128:256]
            else:
                dk_acc[2 * j + c] = jnp.zeros((128, 128), F32)
                dv_acc[2 * j + c] = jnp.zeros((128, 128), F32)
        at += has_dkv[j]

    def per_query(n, tiles):
        def per_key(c, state):
            tiles, odd = state
            gap = (qst[n] - kst[c]) * CHUNK
            seen = gap >= 0

            @pl.when(seen & (odd == 0))
            def _():
                ln[tiles] = n
                l1[tiles] = c
                l2[tiles] = c
                lt1[tiles] = gap
                lt2[tiles] = -100000

            @pl.when(seen & (odd == 1))
            def _():
                l2[tiles] = c
                lt2[tiles] = gap

            step = seen.astype(jnp.int32)
            return tiles + (step & odd), odd ^ step

        tiles, odd = lax.fori_loop(0, nk, per_key, (tiles, jnp.int32(0)), unroll=True)
        return tiles + odd

    tiles = lax.fori_loop(0, nq, per_query, jnp.int32(0))
    for extra in range(UNROLL - 1):
        ln[tiles + extra] = 0
        l1[tiles + extra] = 0
        l2[tiles + extra] = 0
        lt1[tiles + extra] = -100000
        lt2[tiles + extra] = -100000

    line = lax.broadcasted_iota(jnp.int32, (128, 256), 0)
    lane = lax.broadcasted_iota(jnp.int32, (128, 256), 1) & 127
    diff = line - lane

    def tile(t):
        n, c1, c2 = ln[t], l1[t], l2[t]
        k = jnp.concatenate([ks[c1], ks[c2]], axis=0)
        v = jnp.concatenate([vs[c1], vs[c2]], axis=0)
        kt = jnp.concatenate([kts[c1], kts[c2]], axis=1)
        mask = jnp.concatenate([diff - lt1[t], diff - lt2[t]], axis=0) <= 0
        dk = None
        dv = None
        for half in range(2):
            lanes = slice(half * 256, half * 256 + 256)
            more = slice(512 + half * 256, 768 + half * 256)
            q = qc[n, lanes, :]
            do = doc[n, lanes, :]
            scores = dot(k, q, NT) * (SCALE * LOG2E) - rowc[n, 0:1, lanes]
            probs = jnp.where(mask, jnp.exp2(scores), 0.0)
            dprob = dot(v, do, NT)
            dscore = (probs * (dprob * SCALE - rowc[n, 0:1, more])).astype(BF)
            new_v = dot(probs.astype(BF), do, NN)
            new_k = dot(dscore, q, NN)
            dv = new_v if dv is None else dv + new_v
            dk = new_k if dk is None else dk + new_k
            dq_acc[n, :, lanes] += dot(kt, dscore, NN)
        dk_acc[c1] += dk[0:128]
        dv_acc[c1] += dv[0:128]
        dk_acc[c2] += dk[128:256]
        dv_acc[c2] += dv[128:256]

    def turn(i, carry):
        for step in range(UNROLL):
            tile(i * UNROLL + step)
        return carry

    lax.fori_loop(0, (tiles + UNROLL - 1) // UNROLL, turn, 0)

    for b in range(nblocks):
        for c in range(2):
            for h in range(REPEAT):
                rows = slice(h * 128, h * 128 + 128)
                dq_outs[b][rows, c * 128 : c * 128 + 128] = dq_acc[2 * b + c, :, rows].astype(
                    dq_outs[b].dtype
                )
    for j in range(nkv):
        for c in range(2):
            rows = slice(c * 128, c * 128 + 128)
            dkv_outs[j][rows, 0:128] = dk_acc[2 * j + c].astype(dkv_outs[j].dtype)
            dkv_outs[j][rows, 128:256] = dv_acc[2 * j + c].astype(dkv_outs[j].dtype)


def attend(packs, kvs, dq_ins, dkv_ins, dq_types, dkv_types):
    sizes = tuple(p.shape[0] // PIECE for p in packs)
    nq = sum(sizes)
    nk = 2 * len(kvs)
    has_dq = tuple(int(g is not None) for g in dq_ins)
    has_dkv = tuple(int(g is not None) for g in dkv_ins)
    operands = list(packs) + list(kvs) + [g for g in list(dq_ins) + list(dkv_ins) if g is not None]
    most = nq * ((nk + 1) // 2) + UNROLL
    return pl.pallas_call(
        functools.partial(attn_kernel, sizes, len(kvs), has_dq, has_dkv),
        out_shape=tuple(whole((512, ROWS), t) for t in dq_types)
        + tuple(whole((ROWS, 256), t) for t in dkv_types),
        in_specs=[VM] * len(operands),
        out_specs=(VM,) * (len(dq_types) + len(dkv_types)),
        scratch_shapes=[
            pltpu.VMEM((nq, 512, 128), BF),
            pltpu.VMEM((nq, 512, 128), BF),
            pltpu.VMEM((nk, 128, 128), BF),
            pltpu.VMEM((nk, 128, 128), BF),
            pltpu.VMEM((nk, 128, 128), BF),
            pltpu.VMEM((nq, 8, 1024), F32),
            pltpu.VMEM((nq, 128, 512), F32),
            pltpu.VMEM((nk, 128, 128), F32),
            pltpu.VMEM((nk, 128, 128), F32),
            pltpu.SMEM((nq,), jnp.int32),
            pltpu.SMEM((nk,), jnp.int32),
        ]
        + [pltpu.SMEM((most,), jnp.int32)] * 5,
        compiler_params=pltpu.CompilerParams(vmem_limit_bytes=24 * 1024 * 1024),
        cost_estimate=pl.CostEstimate(
            flops=nq * nk * 85_000_000, bytes_accessed=4_000_000, transcendentals=nq * nk * 65536
        ),
    )(*operands)


def rotate(value, cosine, sine):
    first = value[0:HALF]
    second = value[HALF : 2 * HALF]
    return jnp.concatenate(
        [first * cosine + second * sine, second * cosine - first * sine], axis=0
    )


def combine(refs, cos_ref, sin_ref, x_out):
    dqs = refs[0:4]
    dkvs = refs[4:7]
    cosine = cos_ref[...]
    sine = sin_ref[...]
    for head in range(REPEAT):
        rows = slice(head * 128, head * 128 + 128)
        total = dqs[0][rows, :]
        for ref in dqs[1:]:
            total = total + ref[rows, :].astype(F32)
        x_out[rows, :] = rotate(total, cosine, sine).astype(BF)
    total = dkvs[0][...]
    for ref in dkvs[1:]:
        total = total + ref[...].astype(F32)
    x_out[512:640, :] = rotate(total[:, 0:128].T, cosine, sine).astype(BF)
    x_out[640:768, :] = total[:, 128:256].T.astype(BF)


def project(wq_ref, wk_ref, wv_ref, x):
    return (
        dot(wq_ref[...], x[0:512, :], NN)
        + dot(wk_ref[...], x[512:640, :], NN)
        + dot(wv_ref[...], x[640:768, :], NN)
    )


def send_kernel(place, *refs):
    grads = refs[0:7]
    cos_ref, sin_ref, wq_ref, wk_ref, wv_ref, x_out, out_ref = refs[7:]

    @pl.when(pl.program_id(0) == 0)
    def _():
        combine(grads, cos_ref, sin_ref, x_out)

    out_ref[0] = project(wq_ref, wk_ref, wv_ref, x_out).astype(BF)


def keep_kernel(place, x_ref, wq_ref, wk_ref, wv_ref, out_ref):
    out_ref[0] = project(wq_ref, wk_ref, wv_ref, x_ref)


def final_kernel(own_ref, a_ref, b_ref, c_ref, out_ref):
    total = own_ref[...] + a_ref[...].astype(F32) + b_ref[...].astype(F32) + c_ref[...].astype(F32)
    out_ref[...] = total.T.astype(BF)


def whole(shape, dtype):
    return jax.ShapeDtypeStruct(shape, dtype)


VM = pl.BlockSpec(memory_space=pltpu.VMEM)
SM = pl.BlockSpec(memory_space=pltpu.SMEM)


def shards(
    query_act, key_act, value_act, attn_out, out_grad, log_sum, positions, w_query, w_key, w_value
):
    tp = lax.axis_index("tp")
    seq = lax.axis_index("seq")
    core = tp % NC
    xat = tp // NC
    z, y = seq // NY, seq % NY

    pack, kv = pl.pallas_call(
        prep_kernel,
        out_shape=(whole((2 * PIECE, 1024), BF), whole((ROWS + 16, 256), BF)),
        in_specs=[SM] + [VM] * 6,
        out_specs=(VM, VM),
        compiler_params=pltpu.CompilerParams(vmem_limit_bytes=8 * 1024 * 1024),
    )(positions, query_act, out_grad, attn_out, log_sum, key_act, value_act)

    left = move_y(pack, 1)
    right = move_y(pack, -1)
    up1 = move_z(kv, 1)
    down1 = move_z(kv, -1)
    up2 = move_z(up1, 1)
    down2 = move_z(down1, -1)
    up3 = move_z(up2, 1)
    down3 = move_z(down2, -1)
    up4 = move_z(up3, 1)
    far0 = move_y(left[0:PIECE], 1)
    far1 = move_y(right[PIECE : 2 * PIECE], -1)

    near = [kv, up1, down1, up2, down2]
    first = attend([pack, left, right], near, [None] * 3, [None] * 5, [F32] * 3, [F32] * 5)
    second = attend(
        [pack, left, right, far0, far1],
        [up3, down3, up4],
        list(first[0:3]) + [None],
        [None] * 3,
        [F32, BF, BF, F32],
        [F32, BF, BF],
    )
    third = attend([far0, far1], near, [second[3]], list(first[3:8]), [BF], [F32] * 5)

    dqs = [
        second[0],
        move_y(second[1], -1),
        move_y(second[2], 1),
        move_y(third[0], 2),
    ]
    sum_up = move_z(second[6], -1)
    sum_down = move_z(second[5], 1)
    sum_up = move_z((sum_up.astype(F32) + second[4]).astype(BF), -1)
    sum_down = move_z((sum_down.astype(F32) + third[5]).astype(BF), 1)
    sum_up = move_z((sum_up.astype(F32) + third[4]).astype(BF), -1)
    sum_down = move_z((sum_down.astype(F32) + third[3]).astype(BF), 1)
    sum_up = move_z((sum_up.astype(F32) + third[2]).astype(BF), -1)
    dkvs = [third[1], sum_up, sum_down]

    freqs = 500000.0 ** (-(jnp.arange(HALF, dtype=F32) * 2.0 / HEAD_DIM))
    angles = freqs[:, None] * positions.astype(F32)[None, :]
    cosine = jnp.cos(angles)
    sine = jnp.sin(angles)

    place = jnp.stack([xat, core])

    def w_specs(flip):
        def at(i, place):
            return (2 * ((place[0] + i) % NX) + (1 - place[1] if flip else place[1]), 0)

        return [pl.BlockSpec((512, 512), at), pl.BlockSpec((512, 128), at), pl.BlockSpec((512, 128), at)]

    def full(shape):
        return pl.BlockSpec(shape, lambda i, place: (0,) * len(shape))

    out_block = pl.BlockSpec((1, 512, ROWS), lambda i, place: (i, 0, 0))
    grads, to_send = pl.pallas_call(
        send_kernel,
        out_shape=(whole((768, ROWS), BF), whole((4, 512, ROWS), BF)),
        grid_spec=pltpu.PrefetchScalarGridSpec(
            num_scalar_prefetch=1,
            grid=(4,),
            in_specs=[full((512, ROWS))] * 4
            + [full((ROWS, 256))] * 3
            + [full((HALF, ROWS))] * 2
            + w_specs(True),
            out_specs=(full((768, ROWS)), out_block),
        ),
    )(place, *dqs, *dkvs, cosine, sine, w_query, w_key, w_value)
    got = swap_core(to_send)
    kept = pl.pallas_call(
        keep_kernel,
        out_shape=whole((4, 512, ROWS), F32),
        grid_spec=pltpu.PrefetchScalarGridSpec(
            num_scalar_prefetch=1,
            grid=(4,),
            in_specs=[full((768, ROWS))] + w_specs(False),
            out_specs=out_block,
        ),
        cost_estimate=pl.CostEstimate(
            flops=800_000_000, bytes_accessed=4_000_000, transcendentals=0
        ),
    )(place, grads, w_query, w_key, w_value)
    parts = [kept[i] + got[i].astype(F32) for i in range(4)]
    came = [move_x(parts[i].astype(BF), i) for i in (1, 3, 2)]
    return pl.pallas_call(
        final_kernel,
        out_shape=whole((ROWS, 512), BF),
        in_specs=[VM] * 4,
        out_specs=VM,
    )(parts[0], *came)


def solution(mesh):
    return jax.shard_map(
        shards,
        mesh=mesh,
        in_specs=(
            P("seq", "tp"),
            P("seq", "tp"),
            P("seq", "tp"),
            P("seq", "tp"),
            P("seq", "tp"),
            P("tp", "seq"),
            P("seq"),
            P(None, "tp"),
            P(None, "tp"),
            P(None, "tp"),
        ),
        out_specs=P("seq", "tp"),
        check_vma=False,
    )
```

```python
import functools

import jax
import jax.numpy as jnp
from jax import lax
from jax.experimental import pallas as pl
from jax.experimental.pallas import tpu as pltpu
from jax.sharding import PartitionSpec as P

HEADS = 32
KV_HEADS = 8
HEAD_DIM = 128
REPEAT = HEADS // KV_HEADS
HALF = HEAD_DIM // 2
CHUNK = 128
ROWS = 256
NZ, NY, NX, NC = 8, 4, 4, 2
LOG2E = 1.4426950408889634
SCALE = HEAD_DIM**-0.5
BF = jnp.bfloat16
F32 = jnp.float32
PIECE = CHUNK + 16
UNROLL = 2
MIB = 1024 * 1024
PREP_LIMIT = 60 * MIB


def dot(a, b, dims, precision=None):
    return lax.dot_general(
        a, b, (dims, ((), ())), preferred_element_type=F32, precision=precision
    )


NN = ((1,), (0,))
NT = ((1,), (1,))


def move_z(value, steps):
    pairs = [
        (z * NY + y, ((z + steps) % NZ) * NY + y) for z in range(NZ) for y in range(NY)
    ]
    return lax.ppermute(value, "seq", pairs)


def move_y(value, steps):
    pairs = [
        (z * NY + y, z * NY + (y + steps) % NY) for z in range(NZ) for y in range(NY)
    ]
    return lax.ppermute(value, "seq", pairs)


def move_x(value, steps):
    pairs = [
        (x * NC + c, ((x + steps) % NX) * NC + c) for x in range(NX) for c in range(NC)
    ]
    return lax.ppermute(value, "tp", pairs)


def swap_core(value):
    pairs = [(x * NC + c, x * NC + 1 - c) for x in range(NX) for c in range(NC)]
    return lax.ppermute(value, "tp", pairs)


def split3(value):
    high = value.astype(BF)
    rest = value - high.astype(F32)
    mid = rest.astype(BF)
    low = (rest - mid.astype(F32)).astype(BF)
    return high, mid, low


def prep_kernel(pos_hbm, q_hbm, do_hbm, o_hbm, lse_hbm, k_hbm, v_hbm, pack_ref, kv_ref, *scratch):
    pos_ref, o_ref, lse_ref, sems = scratch
    copies = [
        pltpu.make_async_copy(pos_hbm, pos_ref, sems.at[0]),
        pltpu.make_async_copy(lse_hbm, lse_ref, sems.at[1]),
        pltpu.make_async_copy(o_hbm, o_ref, sems.at[2]),
        pltpu.make_async_copy(k_hbm, kv_ref.at[0:ROWS, 0:128], sems.at[3]),
        pltpu.make_async_copy(v_hbm, kv_ref.at[0:ROWS, 128:256], sems.at[4]),
    ]
    for c in range(2):
        rows = slice(c * CHUNK, c * CHUNK + CHUNK)
        into = slice(c * PIECE, c * PIECE + CHUNK)
        copies.append(
            pltpu.make_async_copy(do_hbm.at[rows], pack_ref.at[into, 512:1024], sems.at[5 + c])
        )
        copies.append(
            pltpu.make_async_copy(q_hbm.at[rows], pack_ref.at[into, 0:512], sems.at[7 + c])
        )
    for copy in copies:
        copy.start()
    for copy in copies:
        copy.wait()
    ones = jnp.ones((8, HEAD_DIM), F32)
    index = lax.broadcasted_iota(jnp.int32, (16, 256), 0)
    first = (pos_ref[0] // CHUNK).astype(F32)
    second = (pos_ref[CHUNK] // CHUNK).astype(F32)
    kv_ref[ROWS : ROWS + 16, :] = jnp.where(index == 0, first, second).astype(BF)
    for c in range(2):
        base = c * PIECE
        rows = slice(c * CHUNK, c * CHUNK + CHUNK)
        deltas = []
        for h in range(REPEAT):
            dout = pack_ref[base : base + CHUNK, 512 + h * 128 : 640 + h * 128].astype(F32)
            prod = dout * o_ref[rows, h * 128 : h * 128 + 128].astype(F32)
            deltas.append(dot(ones, prod, NT, lax.Precision.HIGHEST)[0:1])
        lse_row = jnp.concatenate([lse_ref[h : h + 1, rows] for h in range(REPEAT)], axis=1)
        delta_row = jnp.concatenate(deltas, axis=1)
        row = jnp.concatenate([lse_row * LOG2E, delta_row * SCALE], axis=1)
        parts = [part.astype(F32) for part in split3(row)]
        parts.append(jnp.full((1, 1024), second if c else first, F32))
        block = jnp.concatenate(parts + [jnp.zeros((12, 1024), F32)], axis=0)
        pack_ref[base + CHUNK : base + PIECE, :] = block.astype(BF)


def attn_kernel(q_sizes, nkv, has_dq, has_dkv, *refs):
    refs = list(refs)

    def take(count):
        out = refs[:count]
        del refs[:count]
        return out

    packs = take(len(q_sizes))
    kvs = take(nkv)
    dq_ins = take(sum(has_dq))
    dkv_ins = take(sum(has_dkv))
    nblocks = sum(q_sizes) // 2
    dq_outs = take(nblocks)
    dkv_outs = take(nkv)
    qc, doc, ks, vs, kts, rowc, dq_acc, dk_acc, dv_acc, qst, kst, ln, l1, l2, lt1, lt2 = refs
    nq = 2 * nblocks
    nk = 2 * nkv

    n = 0
    for ref, size in zip(packs, q_sizes):
        for c in range(size):
            base = c * PIECE
            meta = ref[base + CHUNK : base + PIECE, :].astype(F32)
            row = meta[0:1] + meta[1:2] + meta[2:3]
            rowc[n] = jnp.broadcast_to(row, (8, 1024))
            qst[n] = jnp.max(meta[3:4, 0:128]).astype(jnp.int32)
            for h in range(REPEAT):
                rows = slice(h * 128, h * 128 + 128)
                qc[n, rows, :] = ref[base : base + CHUNK, h * 128 : h * 128 + 128]
                doc[n, rows, :] = ref[base : base + CHUNK, 512 + h * 128 : 640 + h * 128]
            n += 1
    for j in range(nkv):
        meta = kvs[j][ROWS : ROWS + 16, :].astype(F32)
        for c in range(2):
            rows = slice(c * 128, c * 128 + 128)
            kst[2 * j + c] = jnp.max(meta[c : c + 1, 0:128]).astype(jnp.int32)
            ks[2 * j + c] = kvs[j][rows, 0:128]
            vs[2 * j + c] = kvs[j][rows, 128:256]
            kts[2 * j + c] = kvs[j][rows, 0:128].T
    at = 0
    for b in range(nblocks):
        for c in range(2):
            for h in range(REPEAT):
                lanes = slice(h * 128, h * 128 + 128)
                if has_dq[b]:
                    dq_acc[2 * b + c, :, lanes] = dq_ins[at][lanes, c * 128 : c * 128 + 128]
                else:
                    dq_acc[2 * b + c, :, lanes] = jnp.zeros((128, 128), F32)
        at += has_dq[b]
    at = 0
    for j in range(nkv):
        for c in range(2):
            rows = slice(c * 128, c * 128 + 128)
            if has_dkv[j]:
                dk_acc[2 * j + c] = dkv_ins[at][rows, 0:128]
                dv_acc[2 * j + c] = dkv_ins[at][rows, 128:256]
            else:
                dk_acc[2 * j + c] = jnp.zeros((128, 128), F32)
                dv_acc[2 * j + c] = jnp.zeros((128, 128), F32)
        at += has_dkv[j]

    def per_query(n, tiles):
        def per_key(c, state):
            tiles, odd = state
            gap = (qst[n] - kst[c]) * CHUNK
            seen = gap >= 0

            @pl.when(seen & (odd == 0))
            def _():
                ln[tiles] = n
                l1[tiles] = c
                l2[tiles] = c
                lt1[tiles] = gap
                lt2[tiles] = -100000

            @pl.when(seen & (odd == 1))
            def _():
                l2[tiles] = c
                lt2[tiles] = gap

            step = seen.astype(jnp.int32)
            return tiles + (step & odd), odd ^ step

        tiles, odd = lax.fori_loop(0, nk, per_key, (tiles, jnp.int32(0)), unroll=True)
        return tiles + odd

    tiles = lax.fori_loop(0, nq, per_query, jnp.int32(0))
    for extra in range(UNROLL - 1):
        ln[tiles + extra] = 0
        l1[tiles + extra] = 0
        l2[tiles + extra] = 0
        lt1[tiles + extra] = -100000
        lt2[tiles + extra] = -100000

    line = lax.broadcasted_iota(jnp.int32, (128, 256), 0)
    lane = lax.broadcasted_iota(jnp.int32, (128, 256), 1) & 127
    diff = line - lane

    def load(t):
        n, c1, c2 = ln[t], l1[t], l2[t]
        k = jnp.concatenate([ks[c1], ks[c2]], axis=0)
        v = jnp.concatenate([vs[c1], vs[c2]], axis=0)
        return n, c1, c2, k, v, (lt1[t], lt2[t])

    def opening(unit):
        (n, _, _, k, v, _), half = unit
        lanes = slice(half * 256, half * 256 + 256)
        return dot(k, qc[n, lanes, :], NT), dot(v, doc[n, lanes, :], NT)

    def middle(unit, found):
        (n, _, _, _, _, mask), half = unit
        scores = found[0] * (SCALE * LOG2E) - rowc[n, 0:1, half * 256 : half * 256 + 256]
        probs = jnp.exp2(scores)
        probs = jnp.concatenate(
            [
                jnp.where(diff <= mask[0], probs[0:128], 0.0),
                jnp.where(diff <= mask[1], probs[128:256], 0.0),
            ],
            axis=0,
        )
        dprob = found[1] * SCALE - rowc[n, 0:1, 512 + half * 256 : 768 + half * 256]
        return probs.astype(BF), (probs * dprob).astype(BF)

    def closing(unit, made, sums):
        (n, c1, c2, _, _, _), half = unit
        lanes = slice(half * 256, half * 256 + 256)
        probs, dscore = made
        dv = dot(probs, doc[n, lanes, :], NN)
        dk = dot(dscore, qc[n, lanes, :], NN)
        kt = jnp.concatenate([kts[c1], kts[c2]], axis=1)
        dq_acc[n, :, lanes] += dot(kt, dscore, NN)
        if half == 0:
            return dk, dv
        dk = dk + sums[0]
        dv = dv + sums[1]
        dk_acc[c1] += dk[0:128]
        dv_acc[c1] += dv[0:128]
        dk_acc[c2] += dk[128:256]
        dv_acc[c2] += dv[128:256]
        return None

    def turn(i, carry):
        units = []
        for step in range(UNROLL):
            info = load(i * UNROLL + step)
            units += [(info, 0), (info, 1)]
        found = {0: opening(units[0])}
        sums = None
        made = {}
        for at in range(len(units) + 1):
            if at + 1 < len(units):
                found[at + 1] = opening(units[at + 1])
            if at < len(units):
                made[at] = middle(units[at], found.pop(at))
            if at >= 1:
                sums = closing(units[at - 1], made.pop(at - 1), sums)
        return carry

    lax.fori_loop(0, (tiles + UNROLL - 1) // UNROLL, turn, 0)

    for b in range(nblocks):
        for c in range(2):
            for h in range(REPEAT):
                rows = slice(h * 128, h * 128 + 128)
                dq_outs[b][rows, c * 128 : c * 128 + 128] = dq_acc[2 * b + c, :, rows].astype(
                    dq_outs[b].dtype
                )
    for j in range(nkv):
        for c in range(2):
            rows = slice(c * 128, c * 128 + 128)
            dkv_outs[j][rows, 0:128] = dk_acc[2 * j + c].astype(dkv_outs[j].dtype)
            dkv_outs[j][rows, 128:256] = dv_acc[2 * j + c].astype(dkv_outs[j].dtype)


def attend(packs, kvs, dq_ins, dkv_ins, dq_types, dkv_types):
    sizes = tuple(p.shape[0] // PIECE for p in packs)
    nq = sum(sizes)
    nk = 2 * len(kvs)
    has_dq = tuple(int(g is not None) for g in dq_ins)
    has_dkv = tuple(int(g is not None) for g in dkv_ins)
    operands = list(packs) + list(kvs) + [g for g in list(dq_ins) + list(dkv_ins) if g is not None]
    most = nq * ((nk + 1) // 2) + UNROLL
    return pl.pallas_call(
        functools.partial(attn_kernel, sizes, len(kvs), has_dq, has_dkv),
        out_shape=tuple(whole((512, ROWS), t) for t in dq_types)
        + tuple(whole((ROWS, 256), t) for t in dkv_types),
        in_specs=[VM] * len(operands),
        out_specs=(VM,) * (len(dq_types) + len(dkv_types)),
        scratch_shapes=[
            pltpu.VMEM((nq, 512, 128), BF),
            pltpu.VMEM((nq, 512, 128), BF),
            pltpu.VMEM((nk, 128, 128), BF),
            pltpu.VMEM((nk, 128, 128), BF),
            pltpu.VMEM((nk, 128, 128), BF),
            pltpu.VMEM((nq, 8, 1024), F32),
            pltpu.VMEM((nq, 128, 512), F32),
            pltpu.VMEM((nk, 128, 128), F32),
            pltpu.VMEM((nk, 128, 128), F32),
            pltpu.SMEM((nq,), jnp.int32),
            pltpu.SMEM((nk,), jnp.int32),
        ]
        + [pltpu.SMEM((most,), jnp.int32)] * 5,
        compiler_params=pltpu.CompilerParams(vmem_limit_bytes=28 * MIB),
        cost_estimate=pl.CostEstimate(
            flops=nq * nk * 85_000_000, bytes_accessed=4_000_000, transcendentals=nq * nk * 65536
        ),
    )(*operands)


def rotate(value, cosine, sine):
    first = value[0:HALF]
    second = value[HALF : 2 * HALF]
    return jnp.concatenate(
        [first * cosine + second * sine, second * cosine - first * sine], axis=0
    )


def project(x, weights, i, other):
    tp = lax.axis_index("tp")
    core = tp % NC
    block = NC * lax.rem(tp // NC + i, NX) + (1 - core if other else core)
    rows = pl.ds(pl.multiple_of(block * 512, 512), 512)
    w_query, w_key, w_value = (ref[rows, :] for ref in weights)
    return (
        dot(w_query, x[0:512, :], NN)
        + dot(w_key, x[512:640, :], NN)
        + dot(w_value, x[640:768, :], NN)
    )


def send_kernel(*refs):
    dqs = refs[0:4]
    dkvs = refs[4:12]
    cos_ref, sin_ref, wq_ref, wk_ref, wv_ref, x_out, out_ref = refs[12:]
    cosine = cos_ref[...]
    sine = sin_ref[...]
    for head in range(REPEAT):
        rows = slice(head * 128, head * 128 + 128)
        total = dqs[0][rows, :]
        for ref in dqs[1:]:
            total = total + ref[rows, :].astype(F32)
        x_out[rows, :] = rotate(total, cosine, sine).astype(BF)
    total = dkvs[0][...]
    for ref in dkvs[1:]:
        total = total + ref[...].astype(F32)
    x_out[512:640, :] = rotate(total[:, 0:128].T, cosine, sine).astype(BF)
    x_out[640:768, :] = total[:, 128:256].T.astype(BF)
    for i in range(NX):
        out_ref[i] = project(x_out, (wq_ref, wk_ref, wv_ref), i, True).astype(BF)


def keep_kernel(x_ref, wq_ref, wk_ref, wv_ref, out_ref):
    for i in range(NX):
        out_ref[i] = project(x_ref, (wq_ref, wk_ref, wv_ref), i, False)


def final_kernel(own_ref, a_ref, b_ref, c_ref, out_ref):
    total = own_ref[...] + a_ref[...].astype(F32) + b_ref[...].astype(F32) + c_ref[...].astype(F32)
    out_ref[...] = total.T.astype(BF)


def whole(shape, dtype):
    return jax.ShapeDtypeStruct(shape, dtype)


VM = pl.BlockSpec(memory_space=pltpu.VMEM)
HB = pl.BlockSpec(memory_space=pltpu.HBM)


def shards(
    query_act, key_act, value_act, attn_out, out_grad, log_sum, positions, w_query, w_key, w_value
):
    pack, kv = pl.pallas_call(
        prep_kernel,
        out_shape=(whole((2 * PIECE, 1024), BF), whole((ROWS + 16, 256), BF)),
        in_specs=[HB] * 7,
        out_specs=(VM, VM),
        scratch_shapes=[
            pltpu.SMEM((ROWS,), jnp.int32),
            pltpu.VMEM((ROWS, 512), BF),
            pltpu.VMEM((REPEAT, ROWS), F32),
            pltpu.SemaphoreType.DMA((9,)),
        ],
        compiler_params=pltpu.CompilerParams(vmem_limit_bytes=PREP_LIMIT),
    )(positions, query_act, out_grad, attn_out, log_sum, key_act, value_act)

    left = move_y(pack, 1)
    right = move_y(pack, -1)
    up1 = move_z(kv, 1)
    down1 = move_z(kv, -1)
    up2 = move_z(up1, 1)
    down2 = move_z(down1, -1)
    up3 = move_z(up2, 1)
    down3 = move_z(down2, -1)
    up4 = move_z(up3, 1)
    far0 = move_y(left[0:PIECE], 1)
    far1 = move_y(right[PIECE : 2 * PIECE], -1)

    near = [kv, up1, down1, up2, down2]
    first = attend([pack, left, right], near, [None] * 3, [None] * 5, [F32] * 3, [F32] * 5)
    second = attend(
        [pack, left, right, far0, far1],
        [up3, down3, up4],
        list(first[0:3]) + [None],
        [None] * 3,
        [F32, BF, BF, F32],
        [BF] * 3,
    )
    third = attend([far0, far1], near, [second[3]], list(first[3:8]), [BF], [F32] + [BF] * 4)

    far = [move_z(second[4], -3), move_z(second[5], 3), move_z(second[6], -4)]
    dqs = [
        second[0],
        move_y(second[1], -1),
        move_y(second[2], 1),
        move_y(third[0], 2),
    ]
    close = [move_z(third[2], -1), move_z(third[3], 1), move_z(third[4], -2), move_z(third[5], 2)]
    dkvs = [third[1]] + close + far

    freqs = 500000.0 ** (-(jnp.arange(HALF, dtype=F32) * 2.0 / HEAD_DIM))
    angles = freqs[:, None] * positions.astype(F32)[None, :]
    cosine = jnp.cos(angles)
    sine = jnp.sin(angles)

    grads, to_send = pl.pallas_call(
        send_kernel,
        out_shape=(whole((768, ROWS), BF), whole((NX, 512, ROWS), BF)),
        in_specs=[VM] * 17,
        out_specs=(VM, VM),
        compiler_params=pltpu.CompilerParams(vmem_limit_bytes=20 * MIB),
    )(*dqs, *dkvs, cosine, sine, w_query, w_key, w_value)
    got = swap_core(to_send)
    kept = pl.pallas_call(
        keep_kernel,
        out_shape=whole((NX, 512, ROWS), F32),
        in_specs=[VM] * 4,
        out_specs=VM,
        compiler_params=pltpu.CompilerParams(vmem_limit_bytes=20 * MIB),
        cost_estimate=pl.CostEstimate(
            flops=800_000_000, bytes_accessed=4_000_000, transcendentals=0
        ),
    )(grads, w_query, w_key, w_value)
    parts = [kept[i] + got[i].astype(F32) for i in range(4)]
    came = [move_x(parts[i].astype(BF), i) for i in (1, 3, 2)]
    return pl.pallas_call(
        final_kernel,
        out_shape=whole((ROWS, 512), BF),
        in_specs=[VM] * 4,
        out_specs=VM,
        compiler_params=pltpu.CompilerParams(vmem_limit_bytes=8 * MIB),
    )(parts[0], *came)


def solution(mesh):
    return jax.shard_map(
        shards,
        mesh=mesh,
        in_specs=(
            P("seq", "tp"),
            P("seq", "tp"),
            P("seq", "tp"),
            P("seq", "tp"),
            P("seq", "tp"),
            P("tp", "seq"),
            P("seq"),
            P(None, "tp"),
            P(None, "tp"),
            P(None, "tp"),
        ),
        out_specs=P("seq", "tp"),
        check_vma=False,
    )
```

```python
import functools

import jax
import jax.numpy as jnp
from jax import lax
from jax.experimental import pallas as pl
from jax.experimental.pallas import tpu as pltpu
from jax.sharding import PartitionSpec as P


HEADS = 32
KV_HEADS = 8
HEAD_DIM = 128
REPEAT = HEADS // KV_HEADS
HALF = HEAD_DIM // 2
CHUNK = 128
ROWS = 256
NZ, NY, NX, NC = 8, 4, 4, 2
LOG2E = 1.4426950408889634
SCALE = HEAD_DIM**-0.5
BF = jnp.bfloat16
F32 = jnp.float32
PIECE = CHUNK + 16
UNROLL = 2
MIB = 1024 * 1024
PREP_LIMIT = 60 * MIB


def dot(a, b, dims, precision=None):
    return lax.dot_general(
        a, b, (dims, ((), ())), preferred_element_type=F32, precision=precision
    )


NN = ((1,), (0,))
NT = ((1,), (1,))


def move_z(value, steps):
    pairs = [
        (z * NY + y, ((z + steps) % NZ) * NY + y) for z in range(NZ) for y in range(NY)
    ]
    return lax.ppermute(value, "seq", pairs)


def move_y(value, steps):
    pairs = [
        (z * NY + y, z * NY + (y + steps) % NY) for z in range(NZ) for y in range(NY)
    ]
    return lax.ppermute(value, "seq", pairs)


def move_x(value, steps):
    pairs = [
        (x * NC + c, ((x + steps) % NX) * NC + c) for x in range(NX) for c in range(NC)
    ]
    return lax.ppermute(value, "tp", pairs)


def swap_core(value):
    pairs = [(x * NC + c, x * NC + 1 - c) for x in range(NX) for c in range(NC)]
    return lax.ppermute(value, "tp", pairs)


def split3(value):
    high = value.astype(BF)
    rest = value - high.astype(F32)
    mid = rest.astype(BF)
    low = (rest - mid.astype(F32)).astype(BF)
    return high, mid, low


def prep_kernel(pos_hbm, q_hbm, do_hbm, o_hbm, lse_hbm, k_hbm, v_hbm, pack_ref, kv_ref, *scratch):
    pos_ref, o_ref, lse_ref, sems = scratch
    copies = [
        pltpu.make_async_copy(pos_hbm, pos_ref, sems.at[0]),
        pltpu.make_async_copy(lse_hbm, lse_ref, sems.at[1]),
        pltpu.make_async_copy(o_hbm, o_ref, sems.at[2]),
        pltpu.make_async_copy(k_hbm, kv_ref.at[0:ROWS, 0:128], sems.at[3]),
        pltpu.make_async_copy(v_hbm, kv_ref.at[0:ROWS, 128:256], sems.at[4]),
    ]
    for c in range(2):
        rows = slice(c * CHUNK, c * CHUNK + CHUNK)
        into = slice(c * PIECE, c * PIECE + CHUNK)
        copies.append(
            pltpu.make_async_copy(do_hbm.at[rows], pack_ref.at[into, 512:1024], sems.at[5 + c])
        )
        copies.append(
            pltpu.make_async_copy(q_hbm.at[rows], pack_ref.at[into, 0:512], sems.at[7 + c])
        )
    for copy in copies:
        copy.start()
    for copy in copies:
        copy.wait()
    ones = jnp.ones((8, HEAD_DIM), F32)
    index = lax.broadcasted_iota(jnp.int32, (16, 256), 0)
    first = (pos_ref[0] // CHUNK).astype(F32)
    second = (pos_ref[CHUNK] // CHUNK).astype(F32)
    kv_ref[ROWS : ROWS + 16, :] = jnp.where(index == 0, first, second).astype(BF)
    for c in range(2):
        base = c * PIECE
        rows = slice(c * CHUNK, c * CHUNK + CHUNK)
        deltas = []
        for h in range(REPEAT):
            dout = pack_ref[base : base + CHUNK, 512 + h * 128 : 640 + h * 128].astype(F32)
            prod = dout * o_ref[rows, h * 128 : h * 128 + 128].astype(F32)
            deltas.append(dot(ones, prod, NT, lax.Precision.HIGHEST)[0:1])
        lse_row = jnp.concatenate([lse_ref[h : h + 1, rows] for h in range(REPEAT)], axis=1)
        delta_row = jnp.concatenate(deltas, axis=1)
        row = jnp.concatenate([lse_row * LOG2E, delta_row * SCALE], axis=1)
        parts = [part.astype(F32) for part in split3(row)]
        parts.append(jnp.full((1, 1024), second if c else first, F32))
        block = jnp.concatenate(parts + [jnp.zeros((12, 1024), F32)], axis=0)
        pack_ref[base + CHUNK : base + PIECE, :] = block.astype(BF)


def attn_kernel(q_sizes, nkv, has_dq, has_dkv, layout, *refs):
    refs = list(refs)

    def take(count):
        out = refs[:count]
        del refs[:count]
        return out

    packs = take(len(q_sizes))
    kvs = take(nkv)
    dq_ins = take(sum(has_dq))
    dkv_ins = take(sum(has_dkv))
    nblocks = sum(q_sizes) // 2
    dq_outs = take(nblocks)
    dkv_outs = take(len(layout))
    qc, doc, ks, vs, kts, rowc, dq_acc, dk_acc, dv_acc, qst, kst, ln, l1, l2, lt1, lt2 = refs
    nq = 2 * nblocks
    nk = 2 * nkv

    n = 0
    for ref, size in zip(packs, q_sizes):
        for c in range(size):
            base = c * PIECE
            meta = ref[base + CHUNK : base + PIECE, :].astype(F32)
            row = meta[0:1] + meta[1:2] + meta[2:3]
            rowc[n] = jnp.broadcast_to(row, (8, 1024))
            qst[n] = jnp.max(meta[3:4, 0:128]).astype(jnp.int32)
            for h in range(REPEAT):
                rows = slice(h * 128, h * 128 + 128)
                qc[n, rows, :] = ref[base : base + CHUNK, h * 128 : h * 128 + 128]
                doc[n, rows, :] = ref[base : base + CHUNK, 512 + h * 128 : 640 + h * 128]
            n += 1
    for j in range(nkv):
        meta = kvs[j][ROWS : ROWS + 16, :].astype(F32)
        for c in range(2):
            rows = slice(c * 128, c * 128 + 128)
            kst[2 * j + c] = jnp.max(meta[c : c + 1, 0:128]).astype(jnp.int32)
            ks[2 * j + c] = kvs[j][rows, 0:128]
            vs[2 * j + c] = kvs[j][rows, 128:256]
            kts[2 * j + c] = kvs[j][rows, 0:128].T
    at = 0
    for b in range(nblocks):
        for c in range(2):
            for h in range(REPEAT):
                lanes = slice(h * 128, h * 128 + 128)
                if has_dq[b]:
                    dq_acc[2 * b + c, :, lanes] = dq_ins[at][lanes, c * 128 : c * 128 + 128]
                else:
                    dq_acc[2 * b + c, :, lanes] = jnp.zeros((128, 128), F32)
        at += has_dq[b]
    at = 0
    for j in range(nkv):
        for c in range(2):
            rows = slice(c * 128, c * 128 + 128)
            if has_dkv[j]:
                dk_acc[2 * j + c] = dkv_ins[at][rows, 0:128]
                dv_acc[2 * j + c] = dkv_ins[at][rows, 128:256]
            else:
                dk_acc[2 * j + c] = jnp.zeros((128, 128), F32)
                dv_acc[2 * j + c] = jnp.zeros((128, 128), F32)
        at += has_dkv[j]

    def per_query(n, tiles):
        def per_key(c, state):
            tiles, odd = state
            gap = (qst[n] - kst[c]) * CHUNK
            seen = gap >= 0

            @pl.when(seen & (odd == 0))
            def _():
                ln[tiles] = n
                l1[tiles] = c
                l2[tiles] = c
                lt1[tiles] = gap
                lt2[tiles] = -100000

            @pl.when(seen & (odd == 1))
            def _():
                l2[tiles] = c
                lt2[tiles] = gap

            step = seen.astype(jnp.int32)
            return tiles + (step & odd), odd ^ step

        tiles, odd = lax.fori_loop(0, nk, per_key, (tiles, jnp.int32(0)), unroll=True)
        return tiles + odd

    tiles = lax.fori_loop(0, nq, per_query, jnp.int32(0))
    for extra in range(UNROLL - 1):
        ln[tiles + extra] = 0
        l1[tiles + extra] = 0
        l2[tiles + extra] = 0
        lt1[tiles + extra] = -100000
        lt2[tiles + extra] = -100000

    line = lax.broadcasted_iota(jnp.int32, (128, 256), 0)
    lane = lax.broadcasted_iota(jnp.int32, (128, 256), 1) & 127
    diff = line - lane

    def load(t):
        n, c1, c2 = ln[t], l1[t], l2[t]
        k = jnp.concatenate([ks[c1], ks[c2]], axis=0)
        v = jnp.concatenate([vs[c1], vs[c2]], axis=0)
        return n, c1, c2, k, v, (lt1[t], lt2[t])

    def opening(unit):
        (n, _, _, k, v, _), half = unit
        lanes = slice(half * 256, half * 256 + 256)
        return dot(k, qc[n, lanes, :], NT), dot(v, doc[n, lanes, :], NT)

    def middle(unit, found):
        (n, _, _, _, _, mask), half = unit
        scores = found[0] * (SCALE * LOG2E) - rowc[n, 0:1, half * 256 : half * 256 + 256]
        probs = jnp.exp2(scores)
        probs = jnp.concatenate(
            [
                jnp.where(diff <= mask[0], probs[0:128], 0.0),
                jnp.where(diff <= mask[1], probs[128:256], 0.0),
            ],
            axis=0,
        )
        dprob = found[1] * SCALE - rowc[n, 0:1, 512 + half * 256 : 768 + half * 256]
        return probs.astype(BF), (probs * dprob).astype(BF)

    def closing(unit, made, sums):
        (n, c1, c2, _, _, _), half = unit
        lanes = slice(half * 256, half * 256 + 256)
        probs, dscore = made
        dv = dot(probs, doc[n, lanes, :], NN)
        dk = dot(dscore, qc[n, lanes, :], NN)
        kt = jnp.concatenate([kts[c1], kts[c2]], axis=1)
        dq_acc[n, :, lanes] += dot(kt, dscore, NN)
        if half == 0:
            return dk, dv
        dk = dk + sums[0]
        dv = dv + sums[1]
        dk_acc[c1] += dk[0:128]
        dv_acc[c1] += dv[0:128]
        dk_acc[c2] += dk[128:256]
        dv_acc[c2] += dv[128:256]
        return None

    def turn(i, carry):
        units = []
        for step in range(UNROLL):
            info = load(i * UNROLL + step)
            units += [(info, 0), (info, 1)]
        found = {0: opening(units[0])}
        sums = None
        made = {}
        for at in range(len(units) + 1):
            if at + 1 < len(units):
                found[at + 1] = opening(units[at + 1])
            if at < len(units):
                made[at] = middle(units[at], found.pop(at))
            if at >= 1:
                sums = closing(units[at - 1], made.pop(at - 1), sums)
        return carry

    lax.fori_loop(0, (tiles + UNROLL - 1) // UNROLL, turn, 0)

    for b in range(nblocks):
        for c in range(2):
            for h in range(REPEAT):
                rows = slice(h * 128, h * 128 + 128)
                dq_outs[b][rows, c * 128 : c * 128 + 128] = dq_acc[2 * b + c, :, rows].astype(
                    dq_outs[b].dtype
                )
    for ref, held in zip(dkv_outs, layout):
        for at, c in enumerate(held):
            rows = slice(at * 128, at * 128 + 128)
            ref[rows, 0:128] = dk_acc[c].astype(ref.dtype)
            ref[rows, 128:256] = dv_acc[c].astype(ref.dtype)


def attend(packs, kvs, dq_ins, dkv_ins, dq_types, dkv_types, layout=None):
    layout = layout or tuple((2 * j, 2 * j + 1) for j in range(len(kvs)))
    sizes = tuple(p.shape[0] // PIECE for p in packs)
    nq = sum(sizes)
    nk = 2 * len(kvs)
    has_dq = tuple(int(g is not None) for g in dq_ins)
    has_dkv = tuple(int(g is not None) for g in dkv_ins)
    operands = list(packs) + list(kvs) + [g for g in list(dq_ins) + list(dkv_ins) if g is not None]
    most = nq * ((nk + 1) // 2) + UNROLL
    return pl.pallas_call(
        functools.partial(attn_kernel, sizes, len(kvs), has_dq, has_dkv, layout),
        out_shape=tuple(whole((512, ROWS), t) for t in dq_types)
        + tuple(whole((128 * len(held), 256), t) for held, t in zip(layout, dkv_types)),
        in_specs=[VM] * len(operands),
        out_specs=(VM,) * (len(dq_types) + len(dkv_types)),
        scratch_shapes=[
            pltpu.VMEM((nq, 512, 128), BF),
            pltpu.VMEM((nq, 512, 128), BF),
            pltpu.VMEM((nk, 128, 128), BF),
            pltpu.VMEM((nk, 128, 128), BF),
            pltpu.VMEM((nk, 128, 128), BF),
            pltpu.VMEM((nq, 8, 1024), F32),
            pltpu.VMEM((nq, 128, 512), F32),
            pltpu.VMEM((nk, 128, 128), F32),
            pltpu.VMEM((nk, 128, 128), F32),
            pltpu.SMEM((nq,), jnp.int32),
            pltpu.SMEM((nk,), jnp.int32),
        ]
        + [pltpu.SMEM((most,), jnp.int32)] * 5,
        compiler_params=pltpu.CompilerParams(vmem_limit_bytes=28 * MIB),
        cost_estimate=pl.CostEstimate(
            flops=nq * nk * 85_000_000, bytes_accessed=4_000_000, transcendentals=nq * nk * 65536
        ),
    )(*operands)


def rotate(value, cosine, sine):
    first = value[0:HALF]
    second = value[HALF : 2 * HALF]
    return jnp.concatenate(
        [first * cosine + second * sine, second * cosine - first * sine], axis=0
    )


def project(x, weights, i, other):
    tp = lax.axis_index("tp")
    core = tp % NC
    block = NC * lax.rem(tp // NC + i, NX) + (1 - core if other else core)
    rows = pl.ds(pl.multiple_of(block * 512, 512), 512)
    w_query, w_key, w_value = (ref[rows, :] for ref in weights)
    return (
        dot(w_query, x[0:512, :], NN)
        + dot(w_key, x[512:640, :], NN)
        + dot(w_value, x[640:768, :], NN)
    )


def send_kernel(*refs):
    dqs = refs[0:4]
    dkvs = refs[4:9]
    cos_ref, sin_ref, wq_ref, wk_ref, wv_ref, x_out, out_ref = refs[9:]
    cosine = cos_ref[...]
    sine = sin_ref[...]
    for head in range(REPEAT):
        rows = slice(head * 128, head * 128 + 128)
        total = dqs[0][rows, :]
        for ref in dqs[1:]:
            total = total + ref[rows, :].astype(F32)
        x_out[rows, :] = rotate(total, cosine, sine).astype(BF)
    total = dkvs[0][...]
    for ref in dkvs[1:]:
        total = total + ref[...].astype(F32)
    x_out[512:640, :] = rotate(total[:, 0:128].T, cosine, sine).astype(BF)
    x_out[640:768, :] = total[:, 128:256].T.astype(BF)
    for i in range(NX):
        out_ref[i] = project(x_out, (wq_ref, wk_ref, wv_ref), i, True).astype(BF)


def keep_kernel(x_ref, wq_ref, wk_ref, wv_ref, out_ref):
    for i in range(NX):
        out_ref[i] = project(x_ref, (wq_ref, wk_ref, wv_ref), i, False)


def merge_kernel(up1, down1, up2, down2, from_up, from_down, *outs):
    outs[0][...] = (up1[...] + from_up[0:256, :].astype(F32)).astype(BF)
    outs[1][...] = (down1[...] + from_down[0:256, :].astype(F32)).astype(BF)
    outs[2][0:128, :] = (up2[0:128, :] + from_up[256:384, :].astype(F32)).astype(BF)
    outs[2][128:256, :] = up2[128:256, :].astype(BF)
    outs[3][0:128, :] = down2[0:128, :].astype(BF)
    outs[3][128:256, :] = (down2[128:256, :] + from_down[256:384, :].astype(F32)).astype(BF)


def final_kernel(own_ref, a_ref, b_ref, c_ref, out_ref):
    total = own_ref[...] + a_ref[...].astype(F32) + b_ref[...].astype(F32) + c_ref[...].astype(F32)
    out_ref[...] = total.T.astype(BF)


def whole(shape, dtype):
    return jax.ShapeDtypeStruct(shape, dtype)


VM = pl.BlockSpec(memory_space=pltpu.VMEM)
HB = pl.BlockSpec(memory_space=pltpu.HBM)


def layer(
    query_act, key_act, value_act, attn_out, out_grad, log_sum, positions, w_query, w_key, w_value
):
    pack, kv = pl.pallas_call(
        prep_kernel,
        out_shape=(whole((2 * PIECE, 1024), BF), whole((ROWS + 16, 256), BF)),
        in_specs=[HB] * 7,
        out_specs=(VM, VM),
        scratch_shapes=[
            pltpu.SMEM((ROWS,), jnp.int32),
            pltpu.VMEM((ROWS, 512), BF),
            pltpu.VMEM((REPEAT, ROWS), F32),
            pltpu.SemaphoreType.DMA((9,)),
        ],
        compiler_params=pltpu.CompilerParams(vmem_limit_bytes=PREP_LIMIT),
    )(positions, query_act, out_grad, attn_out, log_sum, key_act, value_act)

    left = move_y(pack, 1)
    right = move_y(pack, -1)
    up1 = move_z(kv, 1)
    down1 = move_z(kv, -1)
    up2 = move_z(up1, 1)
    down2 = move_z(down1, -1)
    up3 = move_z(up2, 1)
    down3 = move_z(down2, -1)
    up4 = move_z(up3, 1)
    far0 = move_y(left[0:PIECE], 1)
    far1 = move_y(right[PIECE : 2 * PIECE], -1)

    near = [kv, up1, down1, up2, down2]
    own = attend([pack], near, [None], [None] * 5, [F32], [F32] * 5)
    side = attend([left, right], near, [None] * 2, list(own[1:]), [F32] * 2, [F32] * 5)
    outer = attend(
        [pack, left, right, far0, far1],
        [up3, down3, up4],
        [own[0], side[0], side[1], None],
        [None] * 3,
        [F32, BF, BF, F32],
        [BF] * 2,
        ((0, 1, 4), (2, 3, 5)),
    )
    back_up = move_z(outer[4], -2)
    back_down = move_z(outer[5], 2)
    last = attend([far0, far1], near, [outer[3]], list(side[2:]), [BF], [F32] * 5)
    dqs = [outer[0], move_y(outer[1], -1), move_y(outer[2], 1), move_y(last[0], 2)]
    merged = pl.pallas_call(
        merge_kernel,
        out_shape=(whole((ROWS, 256), BF),) * 4,
        in_specs=[VM] * 6,
        out_specs=(VM,) * 4,
        compiler_params=pltpu.CompilerParams(vmem_limit_bytes=8 * MIB),
    )(*last[2:6], back_up, back_down)
    dkvs = [last[1]] + [move_z(part, steps) for part, steps in zip(merged, (-1, 1, -2, 2))]

    freqs = 500000.0 ** (-(jnp.arange(HALF, dtype=F32) * 2.0 / HEAD_DIM))
    angles = freqs[:, None] * positions.astype(F32)[None, :]
    cosine = jnp.cos(angles)
    sine = jnp.sin(angles)

    grads, to_send = pl.pallas_call(
        send_kernel,
        out_shape=(whole((768, ROWS), BF), whole((NX, 512, ROWS), BF)),
        in_specs=[VM] * 14,
        out_specs=(VM, VM),
        compiler_params=pltpu.CompilerParams(vmem_limit_bytes=20 * MIB),
    )(*dqs, *dkvs, cosine, sine, w_query, w_key, w_value)
    got = swap_core(to_send)
    kept = pl.pallas_call(
        keep_kernel,
        out_shape=whole((NX, 512, ROWS), F32),
        in_specs=[VM] * 4,
        out_specs=VM,
        compiler_params=pltpu.CompilerParams(vmem_limit_bytes=20 * MIB),
        cost_estimate=pl.CostEstimate(
            flops=800_000_000, bytes_accessed=4_000_000, transcendentals=0
        ),
    )(grads, w_query, w_key, w_value)
    parts = [kept[i] + got[i].astype(F32) for i in range(4)]
    came = [move_x(parts[i].astype(BF), i) for i in (1, 3, 2)]
    return pl.pallas_call(
        final_kernel,
        out_shape=whole((ROWS, 512), BF),
        in_specs=[VM] * 4,
        out_specs=VM,
        compiler_params=pltpu.CompilerParams(vmem_limit_bytes=8 * MIB),
    )(parts[0], *came)


def solution(mesh):
    return jax.shard_map(
        layer,
        mesh=mesh,
        in_specs=(
            P("seq", "tp"),
            P("seq", "tp"),
            P("seq", "tp"),
            P("seq", "tp"),
            P("seq", "tp"),
            P("tp", "seq"),
            P("seq"),
            P(None, "tp"),
            P(None, "tp"),
            P(None, "tp"),
        ),
        out_specs=P("seq", "tp"),
        check_vma=False,
    )
```

```python
import functools

import jax
import jax.numpy as jnp
from jax import lax
from jax.experimental import pallas as pl
from jax.experimental.pallas import tpu as pltpu
from jax.sharding import PartitionSpec as P


HEADS = 32
KV_HEADS = 8
HEAD_DIM = 128
REPEAT = HEADS // KV_HEADS
HALF = HEAD_DIM // 2
CHUNK = 128
ROWS = 256
NZ, NY, NX, NC = 8, 4, 4, 2
LOG2E = 1.4426950408889634
SCALE = HEAD_DIM**-0.5
BF = jnp.bfloat16
F32 = jnp.float32
PIECE = CHUNK + 16
UNROLL = 2
MIB = 1024 * 1024
PREP_LIMIT = 63 * MIB


def dot(a, b, dims, precision=None):
    return lax.dot_general(
        a, b, (dims, ((), ())), preferred_element_type=F32, precision=precision
    )


NN = ((1,), (0,))
NT = ((1,), (1,))


def move_z(value, steps):
    pairs = [
        (z * NY + y, ((z + steps) % NZ) * NY + y) for z in range(NZ) for y in range(NY)
    ]
    return lax.ppermute(value, "seq", pairs)


def move_y(value, steps):
    pairs = [
        (z * NY + y, z * NY + (y + steps) % NY) for z in range(NZ) for y in range(NY)
    ]
    return lax.ppermute(value, "seq", pairs)


def move_x(value, steps):
    pairs = [
        (x * NC + c, ((x + steps) % NX) * NC + c) for x in range(NX) for c in range(NC)
    ]
    return lax.ppermute(value, "tp", pairs)


def swap_core(value):
    pairs = [(x * NC + c, x * NC + 1 - c) for x in range(NX) for c in range(NC)]
    return lax.ppermute(value, "tp", pairs)


def split3(value):
    high = value.astype(BF)
    rest = value - high.astype(F32)
    mid = rest.astype(BF)
    low = (rest - mid.astype(F32)).astype(BF)
    return high, mid, low


def prep_kernel(pos_hbm, q_hbm, do_hbm, o_hbm, lse_hbm, k_hbm, v_hbm, pack_ref, kv_ref, *scratch):
    pos_ref, o_ref, lse_ref, sems = scratch
    copies = [
        pltpu.make_async_copy(pos_hbm, pos_ref, sems.at[0]),
        pltpu.make_async_copy(lse_hbm, lse_ref, sems.at[1]),
        pltpu.make_async_copy(o_hbm, o_ref, sems.at[2]),
        pltpu.make_async_copy(k_hbm, kv_ref.at[0:ROWS, 0:128], sems.at[3]),
        pltpu.make_async_copy(v_hbm, kv_ref.at[0:ROWS, 128:256], sems.at[4]),
    ]
    for c in range(2):
        rows = slice(c * CHUNK, c * CHUNK + CHUNK)
        into = slice(c * PIECE, c * PIECE + CHUNK)
        copies.append(
            pltpu.make_async_copy(do_hbm.at[rows], pack_ref.at[into, 512:1024], sems.at[5 + c])
        )
        copies.append(
            pltpu.make_async_copy(q_hbm.at[rows], pack_ref.at[into, 0:512], sems.at[7 + c])
        )
    for copy in copies:
        copy.start()
    for copy in copies:
        copy.wait()
    ones = jnp.ones((8, HEAD_DIM), F32)
    index = lax.broadcasted_iota(jnp.int32, (16, 256), 0)
    first = (pos_ref[0] // CHUNK).astype(F32)
    second = (pos_ref[CHUNK] // CHUNK).astype(F32)
    kv_ref[ROWS : ROWS + 16, :] = jnp.where(index == 0, first, second).astype(BF)
    for c in range(2):
        base = c * PIECE
        rows = slice(c * CHUNK, c * CHUNK + CHUNK)
        deltas = []
        for h in range(REPEAT):
            dout = pack_ref[base : base + CHUNK, 512 + h * 128 : 640 + h * 128].astype(F32)
            prod = dout * o_ref[rows, h * 128 : h * 128 + 128].astype(F32)
            deltas.append(dot(ones, prod, NT, lax.Precision.HIGHEST)[0:1])
        lse_row = jnp.concatenate([lse_ref[h : h + 1, rows] for h in range(REPEAT)], axis=1)
        delta_row = jnp.concatenate(deltas, axis=1)
        row = jnp.concatenate([lse_row * LOG2E, delta_row * SCALE], axis=1)
        parts = [part.astype(F32) for part in split3(row)]
        parts.append(jnp.full((1, 1024), second if c else first, F32))
        block = jnp.concatenate(parts + [jnp.zeros((12, 1024), F32)], axis=0)
        pack_ref[base + CHUNK : base + PIECE, :] = block.astype(BF)


def stage_kernel(pack_ref, kv_ref, pack_out, kv_out):
    pack_out[...] = pack_ref[...]
    kv_out[...] = kv_ref[...]


def attn_kernel(q_sizes, nkv, has_dq, has_dkv, layout, *refs):
    refs = list(refs)

    def take(count):
        out = refs[:count]
        del refs[:count]
        return out

    packs = take(len(q_sizes))
    kvs = take(nkv)
    dq_ins = take(sum(has_dq))
    dkv_ins = take(sum(has_dkv))
    nblocks = sum(q_sizes) // 2
    dq_outs = take(nblocks)
    dkv_outs = take(len(layout))
    qc, doc, ks, vs, kts, rowc, dq_acc, dk_acc, dv_acc, qst, kst, ln, lc, lg = refs
    nq = 2 * nblocks
    nk = 2 * nkv

    n = 0
    for ref, size in zip(packs, q_sizes):
        for c in range(size):
            base = c * PIECE
            meta = ref[base + CHUNK : base + PIECE, :].astype(F32)
            row = meta[0:1] + meta[1:2] + meta[2:3]
            rowc[n] = jnp.broadcast_to(row, (8, 1024))
            qst[n] = jnp.max(meta[3:4, 0:128]).astype(jnp.int32)
            for h in range(REPEAT):
                rows = slice(h * 128, h * 128 + 128)
                qc[n, rows, :] = ref[base : base + CHUNK, h * 128 : h * 128 + 128]
                doc[n, rows, :] = ref[base : base + CHUNK, 512 + h * 128 : 640 + h * 128]
            n += 1
    for j in range(nkv):
        meta = kvs[j][ROWS : ROWS + 16, :].astype(F32)
        for c in range(2):
            rows = slice(c * 128, c * 128 + 128)
            kst[2 * j + c] = jnp.max(meta[c : c + 1, 0:128]).astype(jnp.int32)
            ks[2 * j + c] = kvs[j][rows, 0:128]
            vs[2 * j + c] = kvs[j][rows, 128:256]
            kts[2 * j + c] = kvs[j][rows, 0:128].T
    at = 0
    for b in range(nblocks):
        for c in range(2):
            for h in range(REPEAT):
                lanes = slice(h * 128, h * 128 + 128)
                if has_dq[b]:
                    dq_acc[2 * b + c, :, lanes] = dq_ins[at][lanes, c * 128 : c * 128 + 128]
                else:
                    dq_acc[2 * b + c, :, lanes] = jnp.zeros((128, 128), F32)
        at += has_dq[b]
    at = 0
    for j in range(nkv):
        for c in range(2):
            rows = slice(c * 128, c * 128 + 128)
            if has_dkv[j]:
                dk_acc[2 * j + c] = dkv_ins[at][rows, 0:128]
                dv_acc[2 * j + c] = dkv_ins[at][rows, 128:256]
            else:
                dk_acc[2 * j + c] = jnp.zeros((128, 128), F32)
                dv_acc[2 * j + c] = jnp.zeros((128, 128), F32)
        at += has_dkv[j]

    def per_query(n, count):
        place = qst[n]
        for c in range(nk):
            gap = (place - kst[c]) * CHUNK
            ln[count] = n
            lc[count] = c
            lg[count] = gap
            count = count + (gap >= 0).astype(jnp.int32)
        ln[count] = n
        lc[count] = 0
        lg[count] = -100000
        return count + (count & 1)

    count = lax.fori_loop(0, nq, per_query, jnp.int32(0))
    for extra in range(2 * UNROLL - 2):
        ln[count + extra] = 0
        lc[count + extra] = 0
        lg[count + extra] = -100000

    line = lax.broadcasted_iota(jnp.int32, (128, 256), 0)
    lane = lax.broadcasted_iota(jnp.int32, (128, 256), 1) & 127
    diff = line - lane

    def load(t):
        n, c1, c2 = ln[2 * t], lc[2 * t], lc[2 * t + 1]
        k = jnp.concatenate([ks[c1], ks[c2]], axis=0)
        v = jnp.concatenate([vs[c1], vs[c2]], axis=0)
        return n, c1, c2, k, v, (lg[2 * t], lg[2 * t + 1])

    def opening(unit):
        (n, _, _, k, v, _), half = unit
        lanes = slice(half * 256, half * 256 + 256)
        return dot(k, qc[n, lanes, :], NT), dot(v, doc[n, lanes, :], NT)

    def middle(unit, found):
        (n, _, _, _, _, mask), half = unit
        scores = found[0] * (SCALE * LOG2E) - rowc[n, 0:1, half * 256 : half * 256 + 256]
        probs = jnp.exp2(scores)
        probs = jnp.concatenate(
            [
                jnp.where(diff <= mask[0], probs[0:128], 0.0),
                jnp.where(diff <= mask[1], probs[128:256], 0.0),
            ],
            axis=0,
        )
        dprob = found[1] * SCALE - rowc[n, 0:1, 512 + half * 256 : 768 + half * 256]
        return probs.astype(BF), (probs * dprob).astype(BF)

    def closing(unit, made, sums):
        (n, c1, c2, _, _, _), half = unit
        lanes = slice(half * 256, half * 256 + 256)
        probs, dscore = made
        dv = dot(probs, doc[n, lanes, :], NN)
        dk = dot(dscore, qc[n, lanes, :], NN)
        kt = jnp.concatenate([kts[c1], kts[c2]], axis=1)
        dq_acc[n, :, lanes] += dot(kt, dscore, NN)
        if half == 0:
            return dk, dv
        dk = dk + sums[0]
        dv = dv + sums[1]
        dk_acc[c1] += dk[0:128]
        dv_acc[c1] += dv[0:128]
        dk_acc[c2] += dk[128:256]
        dv_acc[c2] += dv[128:256]
        return None

    def turn(i, carry):
        units = []
        for step in range(UNROLL):
            info = load(i * UNROLL + step)
            units += [(info, 0), (info, 1)]
        found = {0: opening(units[0])}
        sums = None
        made = {}
        for at in range(len(units) + 1):
            if at + 1 < len(units):
                found[at + 1] = opening(units[at + 1])
            if at < len(units):
                made[at] = middle(units[at], found.pop(at))
            if at >= 1:
                sums = closing(units[at - 1], made.pop(at - 1), sums)
        return carry

    lax.fori_loop(0, (count + 2 * UNROLL - 1) // (2 * UNROLL), turn, 0)

    for b in range(nblocks):
        for c in range(2):
            for h in range(REPEAT):
                rows = slice(h * 128, h * 128 + 128)
                dq_outs[b][rows, c * 128 : c * 128 + 128] = dq_acc[2 * b + c, :, rows].astype(
                    dq_outs[b].dtype
                )
    for ref, held in zip(dkv_outs, layout):
        for at, c in enumerate(held):
            rows = slice(at * 128, at * 128 + 128)
            ref[rows, 0:128] = dk_acc[c].astype(ref.dtype)
            ref[rows, 128:256] = dv_acc[c].astype(ref.dtype)


def attend(packs, kvs, dq_ins, dkv_ins, dq_types, dkv_types, layout=None):
    layout = layout or tuple((2 * j, 2 * j + 1) for j in range(len(kvs)))
    sizes = tuple(p.shape[0] // PIECE for p in packs)
    nq = sum(sizes)
    nk = 2 * len(kvs)
    has_dq = tuple(int(g is not None) for g in dq_ins)
    has_dkv = tuple(int(g is not None) for g in dkv_ins)
    operands = list(packs) + list(kvs) + [g for g in list(dq_ins) + list(dkv_ins) if g is not None]
    most = nq * (nk + 1) + 2 * UNROLL
    return pl.pallas_call(
        functools.partial(attn_kernel, sizes, len(kvs), has_dq, has_dkv, layout),
        out_shape=tuple(whole((512, ROWS), t) for t in dq_types)
        + tuple(whole((128 * len(held), 256), t) for held, t in zip(layout, dkv_types)),
        in_specs=[VM] * len(operands),
        out_specs=(VM,) * (len(dq_types) + len(dkv_types)),
        scratch_shapes=[
            pltpu.VMEM((nq, 512, 128), BF),
            pltpu.VMEM((nq, 512, 128), BF),
            pltpu.VMEM((nk, 128, 128), BF),
            pltpu.VMEM((nk, 128, 128), BF),
            pltpu.VMEM((nk, 128, 128), BF),
            pltpu.VMEM((nq, 8, 1024), F32),
            pltpu.VMEM((nq, 128, 512), F32),
            pltpu.VMEM((nk, 128, 128), F32),
            pltpu.VMEM((nk, 128, 128), F32),
            pltpu.SMEM((nq,), jnp.int32),
            pltpu.SMEM((nk,), jnp.int32),
        ]
        + [pltpu.SMEM((most,), jnp.int32)] * 3,
        compiler_params=pltpu.CompilerParams(vmem_limit_bytes=28 * MIB),
        cost_estimate=pl.CostEstimate(
            flops=nq * nk * 85_000_000, bytes_accessed=4_000_000, transcendentals=nq * nk * 65536
        ),
    )(*operands)


def rotate(value, cosine, sine):
    first = value[0:HALF]
    second = value[HALF : 2 * HALF]
    return jnp.concatenate(
        [first * cosine + second * sine, second * cosine - first * sine], axis=0
    )


def project(x, weights, i, other):
    tp = lax.axis_index("tp")
    core = tp % NC
    block = NC * lax.rem(tp // NC + i, NX) + (1 - core if other else core)
    rows = pl.ds(pl.multiple_of(block * 512, 512), 512)
    w_query, w_key, w_value = (ref[rows, :] for ref in weights)
    return (
        dot(w_query, x[0:512, :], NN)
        + dot(w_key, x[512:640, :], NN)
        + dot(w_value, x[640:768, :], NN)
    )


def send_kernel(*refs):
    dqs = refs[0:4]
    dkvs = refs[4:9]
    cos_ref, sin_ref, wq_ref, wk_ref, wv_ref, x_out, out_ref = refs[9:]
    cosine = cos_ref[...]
    sine = sin_ref[...]
    for head in range(REPEAT):
        rows = slice(head * 128, head * 128 + 128)
        total = dqs[0][rows, :]
        for ref in dqs[1:]:
            total = total + ref[rows, :].astype(F32)
        x_out[rows, :] = rotate(total, cosine, sine).astype(BF)
    total = dkvs[0][...]
    for ref in dkvs[1:]:
        total = total + ref[...].astype(F32)
    x_out[512:640, :] = rotate(total[:, 0:128].T, cosine, sine).astype(BF)
    x_out[640:768, :] = total[:, 128:256].T.astype(BF)
    for i in range(NX):
        out_ref[i] = project(x_out, (wq_ref, wk_ref, wv_ref), i, True).astype(BF)


def keep_kernel(x_ref, wq_ref, wk_ref, wv_ref, out_ref):
    for i in range(NX):
        out_ref[i] = project(x_ref, (wq_ref, wk_ref, wv_ref), i, False)


def merge_kernel(up1, down1, up2, down2, from_up, from_down, *outs):
    outs[0][...] = (up1[...] + from_up[0:256, :].astype(F32)).astype(BF)
    outs[1][...] = (down1[...] + from_down[0:256, :].astype(F32)).astype(BF)
    outs[2][0:128, :] = (up2[0:128, :] + from_up[256:384, :].astype(F32)).astype(BF)
    outs[2][128:256, :] = up2[128:256, :].astype(BF)
    outs[3][0:128, :] = down2[0:128, :].astype(BF)
    outs[3][128:256, :] = (down2[128:256, :] + from_down[256:384, :].astype(F32)).astype(BF)


def final_kernel(own_ref, a_ref, b_ref, c_ref, out_ref):
    total = own_ref[...] + a_ref[...].astype(F32) + b_ref[...].astype(F32) + c_ref[...].astype(F32)
    out_ref[...] = total.T.astype(BF)


def whole(shape, dtype):
    return jax.ShapeDtypeStruct(shape, dtype)


VM = pl.BlockSpec(memory_space=pltpu.VMEM)
HB = pl.BlockSpec(memory_space=pltpu.HBM)


def layer(
    query_act, key_act, value_act, attn_out, out_grad, log_sum, positions, w_query, w_key, w_value
):
    pack, kv = pl.pallas_call(
        prep_kernel,
        out_shape=(whole((2 * PIECE, 1024), BF), whole((ROWS + 16, 256), BF)),
        in_specs=[HB] * 7,
        out_specs=(VM, VM),
        scratch_shapes=[
            pltpu.SMEM((ROWS,), jnp.int32),
            pltpu.VMEM((ROWS, 512), BF),
            pltpu.VMEM((REPEAT, ROWS), F32),
            pltpu.SemaphoreType.DMA((9,)),
        ],
        compiler_params=pltpu.CompilerParams(vmem_limit_bytes=PREP_LIMIT),
    )(positions, query_act, out_grad, attn_out, log_sum, key_act, value_act)

    left = move_y(pack, 1)
    right = move_y(pack, -1)
    up1 = move_z(kv, 1)
    down1 = move_z(kv, -1)
    up2 = move_z(kv, 2)
    down2 = move_z(kv, -2)
    up3 = move_z(up2, 1)
    down3 = move_z(down2, -1)
    up4 = move_z(up2, 2)
    far0 = move_y(left[0:PIECE], 1)
    far1 = move_y(right[PIECE : 2 * PIECE], -1)

    pack, kv = pl.pallas_call(
        stage_kernel,
        out_shape=(whole(pack.shape, BF), whole(kv.shape, BF)),
        in_specs=[VM] * 2,
        out_specs=(VM, VM),
        compiler_params=pltpu.CompilerParams(vmem_limit_bytes=8 * MIB),
    )(pack, kv)
    near = [kv, up1, down1, up2, down2]
    own = attend([pack], near, [None], [None] * 5, [F32], [F32] * 5)
    side = attend([left, right], near, [None] * 2, list(own[1:]), [F32] * 2, [F32] * 5)
    outer = attend(
        [pack, left, right, far0, far1],
        [up3, down3, up4],
        [own[0], side[0], side[1], None],
        [None] * 3,
        [F32, BF, BF, F32],
        [BF] * 2,
        ((0, 1, 4), (2, 3, 5)),
    )
    back_up = move_z(outer[4], -2)
    back_down = move_z(outer[5], 2)
    last = attend([far0, far1], near, [outer[3]], list(side[2:]), [BF], [F32] * 5)
    dqs = [outer[0], move_y(outer[1], -1), move_y(outer[2], 1), move_y(last[0], 2)]
    merged = pl.pallas_call(
        merge_kernel,
        out_shape=(whole((ROWS, 256), BF),) * 4,
        in_specs=[VM] * 6,
        out_specs=(VM,) * 4,
        compiler_params=pltpu.CompilerParams(vmem_limit_bytes=8 * MIB),
    )(*last[2:6], back_up, back_down)
    dkvs = [last[1]] + [move_z(merged[i], steps) for i, steps in ((2, -2), (3, 2), (0, -1), (1, 1))]

    freqs = 500000.0 ** (-(jnp.arange(HALF, dtype=F32) * 2.0 / HEAD_DIM))
    angles = freqs[:, None] * positions.astype(F32)[None, :]
    cosine = jnp.cos(angles)
    sine = jnp.sin(angles)

    grads, to_send = pl.pallas_call(
        send_kernel,
        out_shape=(whole((768, ROWS), BF), whole((NX, 512, ROWS), BF)),
        in_specs=[VM] * 14,
        out_specs=(VM, VM),
        compiler_params=pltpu.CompilerParams(vmem_limit_bytes=20 * MIB),
    )(*dqs, *dkvs, cosine, sine, w_query, w_key, w_value)
    got = swap_core(to_send)
    kept = pl.pallas_call(
        keep_kernel,
        out_shape=whole((NX, 512, ROWS), F32),
        in_specs=[VM] * 4,
        out_specs=VM,
        compiler_params=pltpu.CompilerParams(vmem_limit_bytes=20 * MIB),
        cost_estimate=pl.CostEstimate(
            flops=800_000_000, bytes_accessed=4_000_000, transcendentals=0
        ),
    )(grads, w_query, w_key, w_value)
    parts = [kept[i] + got[i].astype(F32) for i in range(4)]
    came = [move_x(parts[i].astype(BF), i) for i in (2, 1, 3)]
    return pl.pallas_call(
        final_kernel,
        out_shape=whole((ROWS, 512), BF),
        in_specs=[VM] * 4,
        out_specs=VM,
        compiler_params=pltpu.CompilerParams(vmem_limit_bytes=8 * MIB),
    )(parts[0], *came)


def solution(mesh):
    return jax.shard_map(
        layer,
        mesh=mesh,
        in_specs=(
            P("seq", "tp"),
            P("seq", "tp"),
            P("seq", "tp"),
            P("seq", "tp"),
            P("seq", "tp"),
            P("tp", "seq"),
            P("seq"),
            P(None, "tp"),
            P(None, "tp"),
            P(None, "tp"),
        ),
        out_specs=P("seq", "tp"),
        check_vma=False,
    )
```

```python
import functools

import jax
import jax.numpy as jnp
from jax import lax
from jax.experimental import pallas as pl
from jax.experimental.pallas import tpu as pltpu
from jax.sharding import PartitionSpec as P


HEADS = 32
KV_HEADS = 8
HEAD_DIM = 128
REPEAT = HEADS // KV_HEADS
HALF = HEAD_DIM // 2
CHUNK = 128
ROWS = 256
NZ, NY, NX, NC = 8, 4, 4, 2
LOG2E = 1.4426950408889634
SCALE = HEAD_DIM**-0.5
BF = jnp.bfloat16
F32 = jnp.float32
PIECE = CHUNK + 16
UNROLL = 2
MIB = 1024 * 1024
PREP_LIMIT = 63 * MIB


def dot(a, b, dims, precision=None):
    return lax.dot_general(
        a, b, (dims, ((), ())), preferred_element_type=F32, precision=precision
    )


NN = ((1,), (0,))
NT = ((1,), (1,))


def move_z(value, steps):
    pairs = [
        (z * NY + y, ((z + steps) % NZ) * NY + y) for z in range(NZ) for y in range(NY)
    ]
    return lax.ppermute(value, "seq", pairs)


def move_y(value, steps):
    pairs = [
        (z * NY + y, z * NY + (y + steps) % NY) for z in range(NZ) for y in range(NY)
    ]
    return lax.ppermute(value, "seq", pairs)


def move_x(value, steps):
    pairs = [
        (x * NC + c, ((x + steps) % NX) * NC + c) for x in range(NX) for c in range(NC)
    ]
    return lax.ppermute(value, "tp", pairs)


def swap_core(value):
    pairs = [(x * NC + c, x * NC + 1 - c) for x in range(NX) for c in range(NC)]
    return lax.ppermute(value, "tp", pairs)


def split3(value):
    high = value.astype(BF)
    rest = value - high.astype(F32)
    mid = rest.astype(BF)
    low = (rest - mid.astype(F32)).astype(BF)
    return high, mid, low


def prep_kernel(pos_hbm, q_hbm, do_hbm, o_hbm, lse_hbm, k_hbm, v_hbm, pack_ref, kv_ref, *scratch):
    pos_ref, o_ref, lse_ref, sems = scratch
    copies = [
        pltpu.make_async_copy(pos_hbm, pos_ref, sems.at[0]),
        pltpu.make_async_copy(lse_hbm, lse_ref, sems.at[1]),
        pltpu.make_async_copy(o_hbm, o_ref, sems.at[2]),
        pltpu.make_async_copy(k_hbm, kv_ref.at[0:ROWS, 0:128], sems.at[3]),
        pltpu.make_async_copy(v_hbm, kv_ref.at[0:ROWS, 128:256], sems.at[4]),
    ]
    for c in range(2):
        rows = slice(c * CHUNK, c * CHUNK + CHUNK)
        into = slice(c * PIECE, c * PIECE + CHUNK)
        copies.append(
            pltpu.make_async_copy(do_hbm.at[rows], pack_ref.at[into, 512:1024], sems.at[5 + c])
        )
        copies.append(
            pltpu.make_async_copy(q_hbm.at[rows], pack_ref.at[into, 0:512], sems.at[7 + c])
        )
    for copy in copies:
        copy.start()
    for copy in copies:
        copy.wait()
    ones = jnp.ones((8, HEAD_DIM), F32)
    index = lax.broadcasted_iota(jnp.int32, (16, 256), 0)
    first = (pos_ref[0] // CHUNK).astype(F32)
    second = (pos_ref[CHUNK] // CHUNK).astype(F32)
    kv_ref[ROWS : ROWS + 16, :] = jnp.where(index == 0, first, second).astype(BF)
    for c in range(2):
        base = c * PIECE
        rows = slice(c * CHUNK, c * CHUNK + CHUNK)
        deltas = []
        for h in range(REPEAT):
            dout = pack_ref[base : base + CHUNK, 512 + h * 128 : 640 + h * 128].astype(F32)
            prod = dout * o_ref[rows, h * 128 : h * 128 + 128].astype(F32)
            deltas.append(dot(ones, prod, NT, lax.Precision.HIGHEST)[0:1])
        lse_row = jnp.concatenate([lse_ref[h : h + 1, rows] for h in range(REPEAT)], axis=1)
        delta_row = jnp.concatenate(deltas, axis=1)
        row = jnp.concatenate([lse_row * LOG2E, delta_row * SCALE], axis=1)
        parts = [part.astype(F32) for part in split3(row)]
        parts.append(jnp.full((1, 1024), second if c else first, F32))
        block = jnp.concatenate(parts + [jnp.zeros((12, 1024), F32)], axis=0)
        pack_ref[base + CHUNK : base + PIECE, :] = block.astype(BF)


def stage_kernel(pack_ref, kv_ref, pack_out, kv_out):
    pack_out[...] = pack_ref[...]
    kv_out[...] = kv_ref[...]


def attn_kernel(q_sizes, nkv, has_dq, has_dkv, layout, *refs):
    refs = list(refs)

    def take(count):
        out = refs[:count]
        del refs[:count]
        return out

    packs = take(len(q_sizes))
    kvs = take(nkv)
    dq_ins = take(sum(has_dq))
    dkv_ins = take(sum(has_dkv))
    nblocks = sum(q_sizes) // 2
    dq_outs = take(nblocks)
    dkv_outs = take(len(layout))
    qc, doc, ks, vs, kts, rowc, dq_acc, dk_acc, dv_acc, qst, kst, ln, lc, lg = refs
    nq = 2 * nblocks
    nk = 2 * nkv

    n = 0
    for ref, size in zip(packs, q_sizes):
        for c in range(size):
            base = c * PIECE
            meta = ref[base + CHUNK : base + PIECE, :].astype(F32)
            row = meta[0:1] + meta[1:2] + meta[2:3]
            rowc[n] = jnp.broadcast_to(row, (8, 1024))
            qst[n] = jnp.max(meta[3:4, 0:128]).astype(jnp.int32)
            for h in range(REPEAT):
                rows = slice(h * 128, h * 128 + 128)
                qc[n, rows, :] = ref[base : base + CHUNK, h * 128 : h * 128 + 128]
                doc[n, rows, :] = ref[base : base + CHUNK, 512 + h * 128 : 640 + h * 128]
            n += 1
    for j in range(nkv):
        meta = kvs[j][ROWS : ROWS + 16, :].astype(F32)
        for c in range(2):
            rows = slice(c * 128, c * 128 + 128)
            kst[2 * j + c] = jnp.max(meta[c : c + 1, 0:128]).astype(jnp.int32)
            ks[2 * j + c] = kvs[j][rows, 0:128]
            vs[2 * j + c] = kvs[j][rows, 128:256]
            kts[2 * j + c] = kvs[j][rows, 0:128].T
    at = 0
    for b in range(nblocks):
        for c in range(2):
            for h in range(REPEAT):
                lanes = slice(h * 128, h * 128 + 128)
                if has_dq[b]:
                    dq_acc[2 * b + c, :, lanes] = dq_ins[at][lanes, c * 128 : c * 128 + 128]
                else:
                    dq_acc[2 * b + c, :, lanes] = jnp.zeros((128, 128), F32)
        at += has_dq[b]
    at = 0
    for j in range(nkv):
        for c in range(2):
            rows = slice(c * 128, c * 128 + 128)
            if has_dkv[j]:
                dk_acc[2 * j + c] = dkv_ins[at][rows, 0:128]
                dv_acc[2 * j + c] = dkv_ins[at][rows, 128:256]
            else:
                dk_acc[2 * j + c] = jnp.zeros((128, 128), F32)
                dv_acc[2 * j + c] = jnp.zeros((128, 128), F32)
        at += has_dkv[j]

    def per_query(n, count):
        place = qst[n]
        for c in range(nk):
            gap = (place - kst[c]) * CHUNK
            ln[count] = n
            lc[count] = c
            lg[count] = gap
            count = count + (gap >= 0).astype(jnp.int32)
        ln[count] = n
        lc[count] = 0
        lg[count] = -100000
        return count + (count & 1)

    count = lax.fori_loop(0, nq, per_query, jnp.int32(0))
    for extra in range(2 * UNROLL - 2):
        ln[count + extra] = 0
        lc[count + extra] = 0
        lg[count + extra] = -100000

    line = lax.broadcasted_iota(jnp.int32, (128, 256), 0)
    lane = lax.broadcasted_iota(jnp.int32, (128, 256), 1) & 127
    diff = line - lane

    def load(t):
        n, c1, c2 = ln[2 * t], lc[2 * t], lc[2 * t + 1]
        k = jnp.concatenate([ks[c1], ks[c2]], axis=0)
        v = jnp.concatenate([vs[c1], vs[c2]], axis=0)
        return n, c1, c2, k, v, (lg[2 * t], lg[2 * t + 1])

    def opening(unit):
        (n, _, _, k, v, _), half = unit
        lanes = slice(half * 256, half * 256 + 256)
        return dot(k, qc[n, lanes, :], NT), dot(v, doc[n, lanes, :], NT)

    def middle(unit, found):
        (n, _, _, _, _, mask), half = unit
        scores = found[0] * (SCALE * LOG2E) - rowc[n, 0:1, half * 256 : half * 256 + 256]
        probs = jnp.exp2(scores)
        probs = jnp.concatenate(
            [
                jnp.where(diff <= mask[0], probs[0:128], 0.0),
                jnp.where(diff <= mask[1], probs[128:256], 0.0),
            ],
            axis=0,
        )
        dprob = found[1] * SCALE - rowc[n, 0:1, 512 + half * 256 : 768 + half * 256]
        return probs.astype(BF), (probs * dprob).astype(BF)

    def closing(unit, made, sums):
        (n, c1, c2, _, _, _), half = unit
        lanes = slice(half * 256, half * 256 + 256)
        probs, dscore = made
        dv = dot(probs, doc[n, lanes, :], NN)
        dk = dot(dscore, qc[n, lanes, :], NN)
        kt = jnp.concatenate([kts[c1], kts[c2]], axis=1)
        dq_acc[n, :, lanes] += dot(kt, dscore, NN)
        if half == 0:
            return dk, dv
        dk = dk + sums[0]
        dv = dv + sums[1]
        dk_acc[c1] += dk[0:128]
        dv_acc[c1] += dv[0:128]
        dk_acc[c2] += dk[128:256]
        dv_acc[c2] += dv[128:256]
        return None

    def turn(i, carry):
        units = []
        for step in range(UNROLL):
            info = load(i * UNROLL + step)
            units += [(info, 0), (info, 1)]
        found = {0: opening(units[0])}
        sums = None
        made = {}
        for at in range(len(units) + 1):
            if at + 1 < len(units):
                found[at + 1] = opening(units[at + 1])
            if at < len(units):
                made[at] = middle(units[at], found.pop(at))
            if at >= 1:
                sums = closing(units[at - 1], made.pop(at - 1), sums)
        return carry

    lax.fori_loop(0, (count + 2 * UNROLL - 1) // (2 * UNROLL), turn, 0)

    for b in range(nblocks):
        for c in range(2):
            for h in range(REPEAT):
                rows = slice(h * 128, h * 128 + 128)
                dq_outs[b][rows, c * 128 : c * 128 + 128] = dq_acc[2 * b + c, :, rows].astype(
                    dq_outs[b].dtype
                )
    for ref, held in zip(dkv_outs, layout):
        for at, c in enumerate(held):
            rows = slice(at * 128, at * 128 + 128)
            ref[rows, 0:128] = dk_acc[c].astype(ref.dtype)
            ref[rows, 128:256] = dv_acc[c].astype(ref.dtype)


def attend(packs, kvs, dq_ins, dkv_ins, dq_types, dkv_types, layout=None):
    layout = layout or tuple((2 * j, 2 * j + 1) for j in range(len(kvs)))
    sizes = tuple(p.shape[0] // PIECE for p in packs)
    nq = sum(sizes)
    nk = 2 * len(kvs)
    has_dq = tuple(int(g is not None) for g in dq_ins)
    has_dkv = tuple(int(g is not None) for g in dkv_ins)
    operands = list(packs) + list(kvs) + [g for g in list(dq_ins) + list(dkv_ins) if g is not None]
    most = nq * (nk + 1) + 2 * UNROLL
    return pl.pallas_call(
        functools.partial(attn_kernel, sizes, len(kvs), has_dq, has_dkv, layout),
        out_shape=tuple(whole((512, ROWS), t) for t in dq_types)
        + tuple(whole((128 * len(held), 256), t) for held, t in zip(layout, dkv_types)),
        in_specs=[VM] * len(operands),
        out_specs=(VM,) * (len(dq_types) + len(dkv_types)),
        scratch_shapes=[
            pltpu.VMEM((nq, 512, 128), BF),
            pltpu.VMEM((nq, 512, 128), BF),
            pltpu.VMEM((nk, 128, 128), BF),
            pltpu.VMEM((nk, 128, 128), BF),
            pltpu.VMEM((nk, 128, 128), BF),
            pltpu.VMEM((nq, 8, 1024), F32),
            pltpu.VMEM((nq, 128, 512), F32),
            pltpu.VMEM((nk, 128, 128), F32),
            pltpu.VMEM((nk, 128, 128), F32),
            pltpu.SMEM((nq,), jnp.int32),
            pltpu.SMEM((nk,), jnp.int32),
        ]
        + [pltpu.SMEM((most,), jnp.int32)] * 3,
        compiler_params=pltpu.CompilerParams(vmem_limit_bytes=28 * MIB),
        cost_estimate=pl.CostEstimate(
            flops=nq * nk * 85_000_000, bytes_accessed=4_000_000, transcendentals=nq * nk * 65536
        ),
    )(*operands)


def rotate(value, cosine, sine):
    first = value[0:HALF]
    second = value[HALF : 2 * HALF]
    return jnp.concatenate(
        [first * cosine + second * sine, second * cosine - first * sine], axis=0
    )


def project(x, weights, i, other):
    tp = lax.axis_index("tp")
    core = tp % NC
    block = NC * lax.rem(tp // NC + i, NX) + (1 - core if other else core)
    rows = pl.ds(pl.multiple_of(block * 512, 512), 512)
    w_query, w_key, w_value = (ref[rows, :] for ref in weights)
    return (
        dot(w_query, x[0:512, :], NN)
        + dot(w_key, x[512:640, :], NN)
        + dot(w_value, x[640:768, :], NN)
    )


def send_kernel(*refs):
    dqs = refs[0:4]
    dkvs = refs[4:9]
    cos_ref, sin_ref, wq_ref, wk_ref, wv_ref, x_out, out_ref = refs[9:]
    cosine = cos_ref[...]
    sine = sin_ref[...]
    for head in range(REPEAT):
        rows = slice(head * 128, head * 128 + 128)
        total = dqs[0][rows, :]
        for ref in dqs[1:]:
            total = total + ref[rows, :].astype(F32)
        x_out[rows, :] = rotate(total, cosine, sine).astype(BF)
    total = dkvs[0][...]
    for ref in dkvs[1:]:
        total = total + ref[...].astype(F32)
    x_out[512:640, :] = rotate(total[:, 0:128].T, cosine, sine).astype(BF)
    x_out[640:768, :] = total[:, 128:256].T.astype(BF)
    for i in range(NX):
        out_ref[i] = project(x_out, (wq_ref, wk_ref, wv_ref), i, True).astype(BF)


def keep_kernel(x_ref, wq_ref, wk_ref, wv_ref, out_ref):
    for i in range(NX):
        out_ref[i] = project(x_ref, (wq_ref, wk_ref, wv_ref), i, False)


def merge_kernel(up1, down1, up2, down2, from_up, from_down, *outs):
    outs[0][...] = (up1[...] + from_up[0:256, :].astype(F32)).astype(BF)
    outs[1][...] = (down1[...] + from_down[0:256, :].astype(F32)).astype(BF)
    outs[2][0:128, :] = (up2[0:128, :] + from_up[256:384, :].astype(F32)).astype(BF)
    outs[2][128:256, :] = up2[128:256, :].astype(BF)
    outs[3][0:128, :] = down2[0:128, :].astype(BF)
    outs[3][128:256, :] = (down2[128:256, :] + from_down[256:384, :].astype(F32)).astype(BF)


def final_kernel(own_ref, a_ref, b_ref, c_ref, out_ref):
    total = own_ref[...] + a_ref[...].astype(F32) + b_ref[...].astype(F32) + c_ref[...].astype(F32)
    out_ref[...] = total.T.astype(BF)


def whole(shape, dtype):
    return jax.ShapeDtypeStruct(shape, dtype)


VM = pl.BlockSpec(memory_space=pltpu.VMEM)
HB = pl.BlockSpec(memory_space=pltpu.HBM)


def layer(
    query_act, key_act, value_act, attn_out, out_grad, log_sum, positions, w_query, w_key, w_value
):
    pack, kv = pl.pallas_call(
        prep_kernel,
        out_shape=(whole((2 * PIECE, 1024), BF), whole((ROWS + 16, 256), BF)),
        in_specs=[HB] * 7,
        out_specs=(VM, VM),
        scratch_shapes=[
            pltpu.SMEM((ROWS,), jnp.int32),
            pltpu.VMEM((ROWS, 512), BF),
            pltpu.VMEM((REPEAT, ROWS), F32),
            pltpu.SemaphoreType.DMA((9,)),
        ],
        compiler_params=pltpu.CompilerParams(vmem_limit_bytes=PREP_LIMIT),
    )(positions, query_act, out_grad, attn_out, log_sum, key_act, value_act)

    left = move_y(pack, 1)
    right = move_y(pack, -1)
    up1 = move_z(kv, 1)
    down1 = move_z(kv, -1)
    up2 = move_z(kv, 2)
    down2 = move_z(kv, -2)
    up3 = move_z(up2, 1)
    down3 = move_z(down2, -1)
    up4 = move_z(up2, 2)
    far = move_y(pack, 2)

    pack, kv = pl.pallas_call(
        stage_kernel,
        out_shape=(whole(pack.shape, BF), whole(kv.shape, BF)),
        in_specs=[VM] * 2,
        out_specs=(VM, VM),
        compiler_params=pltpu.CompilerParams(vmem_limit_bytes=8 * MIB),
    )(pack, kv)
    near = [kv, up1, down1, up2, down2]
    first = attend([pack, left, right], near, [None] * 3, [None] * 5, [F32] * 3, [F32] * 5)
    outer = attend(
        [pack, left, right, far],
        [up3, down3, up4],
        list(first[0:3]) + [None],
        [None] * 3,
        [F32, BF, BF, F32],
        [BF] * 2,
        ((0, 1, 4), (2, 3, 5)),
    )
    back_up = move_z(outer[4], -2)
    back_down = move_z(outer[5], 2)
    last = attend([far], near, [outer[3]], list(first[3:8]), [BF], [F32] * 5)
    dqs = [outer[0], move_y(outer[1], -1), move_y(outer[2], 1), move_y(last[0], 2)]
    merged = pl.pallas_call(
        merge_kernel,
        out_shape=(whole((ROWS, 256), BF),) * 4,
        in_specs=[VM] * 6,
        out_specs=(VM,) * 4,
        compiler_params=pltpu.CompilerParams(vmem_limit_bytes=8 * MIB),
    )(*last[2:6], back_up, back_down)
    dkvs = [last[1]] + [move_z(merged[i], steps) for i, steps in ((2, -2), (3, 2), (0, -1), (1, 1))]

    freqs = 500000.0 ** (-(jnp.arange(HALF, dtype=F32) * 2.0 / HEAD_DIM))
    angles = freqs[:, None] * positions.astype(F32)[None, :]
    cosine = jnp.cos(angles)
    sine = jnp.sin(angles)

    grads, to_send = pl.pallas_call(
        send_kernel,
        out_shape=(whole((768, ROWS), BF), whole((NX, 512, ROWS), BF)),
        in_specs=[VM] * 14,
        out_specs=(VM, VM),
        compiler_params=pltpu.CompilerParams(vmem_limit_bytes=20 * MIB),
    )(*dqs, *dkvs, cosine, sine, w_query, w_key, w_value)
    got = swap_core(to_send)
    kept = pl.pallas_call(
        keep_kernel,
        out_shape=whole((NX, 512, ROWS), F32),
        in_specs=[VM] * 4,
        out_specs=VM,
        compiler_params=pltpu.CompilerParams(vmem_limit_bytes=20 * MIB),
        cost_estimate=pl.CostEstimate(
            flops=800_000_000, bytes_accessed=4_000_000, transcendentals=0
        ),
    )(grads, w_query, w_key, w_value)
    parts = [kept[i] + got[i].astype(F32) for i in range(4)]
    came = [move_x(parts[i].astype(BF), i) for i in (2, 1, 3)]
    return pl.pallas_call(
        final_kernel,
        out_shape=whole((ROWS, 512), BF),
        in_specs=[VM] * 4,
        out_specs=VM,
        compiler_params=pltpu.CompilerParams(vmem_limit_bytes=8 * MIB),
    )(parts[0], *came)


def solution(mesh):
    return jax.shard_map(
        layer,
        mesh=mesh,
        in_specs=(
            P("seq", "tp"),
            P("seq", "tp"),
            P("seq", "tp"),
            P("seq", "tp"),
            P("seq", "tp"),
            P("tp", "seq"),
            P("seq"),
            P(None, "tp"),
            P(None, "tp"),
            P(None, "tp"),
        ),
        out_specs=P("seq", "tp"),
        check_vma=False,
    )
```

```python
import functools

import jax
import jax.numpy as jnp
from jax import lax
from jax.experimental import pallas as pl
from jax.experimental.pallas import tpu as pltpu
from jax.sharding import PartitionSpec as P


HEADS = 32
KV_HEADS = 8
HEAD_DIM = 128
REPEAT = HEADS // KV_HEADS
HALF = HEAD_DIM // 2
CHUNK = 128
ROWS = 256
NZ, NY, NX, NC = 8, 4, 4, 2
LOG2E = 1.4426950408889634
SCALE = HEAD_DIM**-0.5
BF = jnp.bfloat16
F32 = jnp.float32
PIECE = CHUNK + 16
UNROLL = 2
MIB = 1024 * 1024
PREP_LIMIT = 63 * MIB


def dot(a, b, dims, precision=None):
    return lax.dot_general(
        a, b, (dims, ((), ())), preferred_element_type=F32, precision=precision
    )


NN = ((1,), (0,))
NT = ((1,), (1,))


def move_z(value, steps):
    pairs = [
        (z * NY + y, ((z + steps) % NZ) * NY + y) for z in range(NZ) for y in range(NY)
    ]
    return lax.ppermute(value, "seq", pairs)


def move_y(value, steps):
    pairs = [
        (z * NY + y, z * NY + (y + steps) % NY) for z in range(NZ) for y in range(NY)
    ]
    return lax.ppermute(value, "seq", pairs)


def move_x(value, steps):
    pairs = [
        (x * NC + c, ((x + steps) % NX) * NC + c) for x in range(NX) for c in range(NC)
    ]
    return lax.ppermute(value, "tp", pairs)


def swap_core(value):
    pairs = [(x * NC + c, x * NC + 1 - c) for x in range(NX) for c in range(NC)]
    return lax.ppermute(value, "tp", pairs)


def split3(value):
    high = value.astype(BF)
    rest = value - high.astype(F32)
    mid = rest.astype(BF)
    low = (rest - mid.astype(F32)).astype(BF)
    return high, mid, low


def prep_kernel(
    pos_hbm, q_hbm, do_hbm, o_hbm, lse_hbm, k_hbm, v_hbm, pack_ref, kv_ref, mark_ref, *scratch
):
    mark_ref[...] = jnp.zeros_like(mark_ref)
    pos_ref, o_ref, lse_ref, sems = scratch
    copies = [
        pltpu.make_async_copy(pos_hbm, pos_ref, sems.at[0]),
        pltpu.make_async_copy(lse_hbm, lse_ref, sems.at[1]),
        pltpu.make_async_copy(o_hbm, o_ref, sems.at[2]),
        pltpu.make_async_copy(k_hbm, kv_ref.at[0:ROWS, 0:128], sems.at[3]),
        pltpu.make_async_copy(v_hbm, kv_ref.at[0:ROWS, 128:256], sems.at[4]),
    ]
    for c in range(2):
        rows = slice(c * CHUNK, c * CHUNK + CHUNK)
        into = slice(c * PIECE, c * PIECE + CHUNK)
        copies.append(
            pltpu.make_async_copy(do_hbm.at[rows], pack_ref.at[into, 512:1024], sems.at[5 + c])
        )
        copies.append(
            pltpu.make_async_copy(q_hbm.at[rows], pack_ref.at[into, 0:512], sems.at[7 + c])
        )
    for copy in copies:
        copy.start()
    for copy in copies:
        copy.wait()
    ones = jnp.ones((8, HEAD_DIM), F32)
    index = lax.broadcasted_iota(jnp.int32, (16, 256), 0)
    first = (pos_ref[0] // CHUNK).astype(F32)
    second = (pos_ref[CHUNK] // CHUNK).astype(F32)
    kv_ref[ROWS : ROWS + 16, :] = jnp.where(index == 0, first, second).astype(BF)
    for c in range(2):
        base = c * PIECE
        rows = slice(c * CHUNK, c * CHUNK + CHUNK)
        deltas = []
        for h in range(REPEAT):
            dout = pack_ref[base : base + CHUNK, 512 + h * 128 : 640 + h * 128].astype(F32)
            prod = dout * o_ref[rows, h * 128 : h * 128 + 128].astype(F32)
            deltas.append(dot(ones, prod, NT, lax.Precision.HIGHEST)[0:1])
        lse_row = jnp.concatenate([lse_ref[h : h + 1, rows] for h in range(REPEAT)], axis=1)
        delta_row = jnp.concatenate(deltas, axis=1)
        row = jnp.concatenate([lse_row * LOG2E, delta_row * SCALE], axis=1)
        parts = [part.astype(F32) for part in split3(row)]
        parts.append(jnp.full((1, 1024), second if c else first, F32))
        block = jnp.concatenate(parts + [jnp.zeros((12, 1024), F32)], axis=0)
        pack_ref[base + CHUNK : base + PIECE, :] = block.astype(BF)


def pause_kernel(mark_ref, out_ref):
    del mark_ref, out_ref


def attn_kernel(q_sizes, nkv, has_dq, has_dkv, layout, *refs):
    refs = list(refs)

    def take(count):
        out = refs[:count]
        del refs[:count]
        return out

    packs = take(len(q_sizes))
    kvs = take(nkv)
    dq_ins = take(sum(has_dq))
    dkv_ins = take(sum(has_dkv))
    nblocks = sum(q_sizes) // 2
    dq_outs = take(nblocks)
    dkv_outs = take(len(layout))
    qc, doc, ks, vs, kts, rowc, dq_acc, dk_acc, dv_acc, qst, kst, ln, lc, lg = refs
    nq = 2 * nblocks
    nk = 2 * nkv

    n = 0
    for ref, size in zip(packs, q_sizes):
        for c in range(size):
            base = c * PIECE
            meta = ref[base + CHUNK : base + PIECE, :].astype(F32)
            row = meta[0:1] + meta[1:2] + meta[2:3]
            rowc[n] = jnp.broadcast_to(row, (8, 1024))
            qst[n] = jnp.max(meta[3:4, 0:128]).astype(jnp.int32)
            for h in range(REPEAT):
                rows = slice(h * 128, h * 128 + 128)
                qc[n, rows, :] = ref[base : base + CHUNK, h * 128 : h * 128 + 128]
                doc[n, rows, :] = ref[base : base + CHUNK, 512 + h * 128 : 640 + h * 128]
            n += 1
    for j in range(nkv):
        meta = kvs[j][ROWS : ROWS + 16, :].astype(F32)
        for c in range(2):
            rows = slice(c * 128, c * 128 + 128)
            kst[2 * j + c] = jnp.max(meta[c : c + 1, 0:128]).astype(jnp.int32)
            ks[2 * j + c] = kvs[j][rows, 0:128]
            vs[2 * j + c] = kvs[j][rows, 128:256]
            kts[2 * j + c] = kvs[j][rows, 0:128].T
    at = 0
    for b in range(nblocks):
        for c in range(2):
            for h in range(REPEAT):
                lanes = slice(h * 128, h * 128 + 128)
                if has_dq[b]:
                    dq_acc[2 * b + c, :, lanes] = dq_ins[at][lanes, c * 128 : c * 128 + 128]
                else:
                    dq_acc[2 * b + c, :, lanes] = jnp.zeros((128, 128), F32)
        at += has_dq[b]
    at = 0
    for j in range(nkv):
        for c in range(2):
            rows = slice(c * 128, c * 128 + 128)
            if has_dkv[j]:
                dk_acc[2 * j + c] = dkv_ins[at][rows, 0:128]
                dv_acc[2 * j + c] = dkv_ins[at][rows, 128:256]
            else:
                dk_acc[2 * j + c] = jnp.zeros((128, 128), F32)
                dv_acc[2 * j + c] = jnp.zeros((128, 128), F32)
        at += has_dkv[j]

    def per_query(n, count):
        place = qst[n]
        for c in range(nk):
            gap = (place - kst[c]) * CHUNK
            ln[count] = n
            lc[count] = c
            lg[count] = gap
            count = count + (gap >= 0).astype(jnp.int32)
        ln[count] = n
        lc[count] = 0
        lg[count] = -100000
        return count + (count & 1)

    count = lax.fori_loop(0, nq, per_query, jnp.int32(0))
    for extra in range(2 * UNROLL - 2):
        ln[count + extra] = 0
        lc[count + extra] = 0
        lg[count + extra] = -100000

    line = lax.broadcasted_iota(jnp.int32, (128, 256), 0)
    lane = lax.broadcasted_iota(jnp.int32, (128, 256), 1) & 127
    diff = line - lane

    def load(t):
        n, c1, c2 = ln[2 * t], lc[2 * t], lc[2 * t + 1]
        k = jnp.concatenate([ks[c1], ks[c2]], axis=0)
        v = jnp.concatenate([vs[c1], vs[c2]], axis=0)
        return n, c1, c2, k, v, (lg[2 * t], lg[2 * t + 1])

    def opening(unit):
        (n, _, _, k, v, _), half = unit
        lanes = slice(half * 256, half * 256 + 256)
        return dot(k, qc[n, lanes, :], NT), dot(v, doc[n, lanes, :], NT)

    def middle(unit, found):
        (n, _, _, _, _, mask), half = unit
        scores = found[0] * (SCALE * LOG2E) - rowc[n, 0:1, half * 256 : half * 256 + 256]
        probs = jnp.exp2(scores)
        probs = jnp.concatenate(
            [
                jnp.where(diff <= mask[0], probs[0:128], 0.0),
                jnp.where(diff <= mask[1], probs[128:256], 0.0),
            ],
            axis=0,
        )
        dprob = found[1] * SCALE - rowc[n, 0:1, 512 + half * 256 : 768 + half * 256]
        return probs.astype(BF), (probs * dprob).astype(BF)

    def closing(unit, made, sums):
        (n, c1, c2, _, _, _), half = unit
        lanes = slice(half * 256, half * 256 + 256)
        probs, dscore = made
        dv = dot(probs, doc[n, lanes, :], NN)
        dk = dot(dscore, qc[n, lanes, :], NN)
        kt = jnp.concatenate([kts[c1], kts[c2]], axis=1)
        dq_acc[n, :, lanes] += dot(kt, dscore, NN)
        if half == 0:
            return dk, dv
        dk = dk + sums[0]
        dv = dv + sums[1]
        dk_acc[c1] += dk[0:128]
        dv_acc[c1] += dv[0:128]
        dk_acc[c2] += dk[128:256]
        dv_acc[c2] += dv[128:256]
        return None

    def turn(i, carry):
        units = []
        for step in range(UNROLL):
            info = load(i * UNROLL + step)
            units += [(info, 0), (info, 1)]
        found = {0: opening(units[0])}
        sums = None
        made = {}
        for at in range(len(units) + 1):
            if at + 1 < len(units):
                found[at + 1] = opening(units[at + 1])
            if at < len(units):
                made[at] = middle(units[at], found.pop(at))
            if at >= 1:
                sums = closing(units[at - 1], made.pop(at - 1), sums)
        return carry

    lax.fori_loop(0, (count + 2 * UNROLL - 1) // (2 * UNROLL), turn, 0)

    for b in range(nblocks):
        for c in range(2):
            for h in range(REPEAT):
                rows = slice(h * 128, h * 128 + 128)
                dq_outs[b][rows, c * 128 : c * 128 + 128] = dq_acc[2 * b + c, :, rows].astype(
                    dq_outs[b].dtype
                )
    for ref, held in zip(dkv_outs, layout):
        for at, c in enumerate(held):
            rows = slice(at * 128, at * 128 + 128)
            ref[rows, 0:128] = dk_acc[c].astype(ref.dtype)
            ref[rows, 128:256] = dv_acc[c].astype(ref.dtype)


def attend(packs, kvs, dq_ins, dkv_ins, dq_types, dkv_types, layout=None):
    layout = layout or tuple((2 * j, 2 * j + 1) for j in range(len(kvs)))
    sizes = tuple(p.shape[0] // PIECE for p in packs)
    nq = sum(sizes)
    nk = 2 * len(kvs)
    has_dq = tuple(int(g is not None) for g in dq_ins)
    has_dkv = tuple(int(g is not None) for g in dkv_ins)
    operands = list(packs) + list(kvs) + [g for g in list(dq_ins) + list(dkv_ins) if g is not None]
    most = nq * (nk + 1) + 2 * UNROLL
    return pl.pallas_call(
        functools.partial(attn_kernel, sizes, len(kvs), has_dq, has_dkv, layout),
        out_shape=tuple(whole((512, ROWS), t) for t in dq_types)
        + tuple(whole((128 * len(held), 256), t) for held, t in zip(layout, dkv_types)),
        in_specs=[VM] * len(operands),
        out_specs=(VM,) * (len(dq_types) + len(dkv_types)),
        scratch_shapes=[
            pltpu.VMEM((nq, 512, 128), BF),
            pltpu.VMEM((nq, 512, 128), BF),
            pltpu.VMEM((nk, 128, 128), BF),
            pltpu.VMEM((nk, 128, 128), BF),
            pltpu.VMEM((nk, 128, 128), BF),
            pltpu.VMEM((nq, 8, 1024), F32),
            pltpu.VMEM((nq, 128, 512), F32),
            pltpu.VMEM((nk, 128, 128), F32),
            pltpu.VMEM((nk, 128, 128), F32),
            pltpu.SMEM((nq,), jnp.int32),
            pltpu.SMEM((nk,), jnp.int32),
        ]
        + [pltpu.SMEM((most,), jnp.int32)] * 3,
        compiler_params=pltpu.CompilerParams(vmem_limit_bytes=28 * MIB),
        cost_estimate=pl.CostEstimate(
            flops=nq * nk * 85_000_000, bytes_accessed=4_000_000, transcendentals=nq * nk * 65536
        ),
    )(*operands)


def rotate(value, cosine, sine):
    first = value[0:HALF]
    second = value[HALF : 2 * HALF]
    return jnp.concatenate(
        [first * cosine + second * sine, second * cosine - first * sine], axis=0
    )


def project(x, weights, i, other):
    tp = lax.axis_index("tp")
    core = tp % NC
    block = NC * lax.rem(tp // NC + i, NX) + (1 - core if other else core)
    rows = pl.ds(pl.multiple_of(block * 512, 512), 512)
    w_query, w_key, w_value = (ref[rows, :] for ref in weights)
    return (
        dot(w_query, x[0:512, :], NN)
        + dot(w_key, x[512:640, :], NN)
        + dot(w_value, x[640:768, :], NN)
    )


def send_kernel(*refs):
    dqs = refs[0:4]
    dkvs = refs[4:9]
    cos_ref, sin_ref, wq_ref, wk_ref, wv_ref, _, x_out, out_ref = refs[9:]
    cosine = cos_ref[...]
    sine = sin_ref[...]
    for head in range(REPEAT):
        rows = slice(head * 128, head * 128 + 128)
        total = dqs[0][rows, :]
        for ref in dqs[1:]:
            total = total + ref[rows, :].astype(F32)
        x_out[rows, :] = rotate(total, cosine, sine).astype(BF)
    total = dkvs[0][...]
    for ref in dkvs[1:]:
        total = total + ref[...].astype(F32)
    x_out[512:640, :] = rotate(total[:, 0:128].T, cosine, sine).astype(BF)
    x_out[640:768, :] = total[:, 128:256].T.astype(BF)
    for i in range(NX):
        out_ref[i] = project(x_out, (wq_ref, wk_ref, wv_ref), i, True).astype(BF)


def keep_kernel(x_ref, wq_ref, wk_ref, wv_ref, out_ref):
    for i in range(NX):
        out_ref[i] = project(x_ref, (wq_ref, wk_ref, wv_ref), i, False)


def merge_kernel(up1, down1, up2, down2, from_up, from_down, *outs):
    outs[0][...] = (up1[...] + from_up[0:256, :].astype(F32)).astype(BF)
    outs[1][...] = (down1[...] + from_down[0:256, :].astype(F32)).astype(BF)
    outs[2][0:128, :] = (up2[0:128, :] + from_up[256:384, :].astype(F32)).astype(BF)
    outs[2][128:256, :] = up2[128:256, :].astype(BF)
    outs[3][0:128, :] = down2[0:128, :].astype(BF)
    outs[3][128:256, :] = (down2[128:256, :] + from_down[256:384, :].astype(F32)).astype(BF)


def final_kernel(own_ref, a_ref, b_ref, c_ref, out_ref):
    total = own_ref[...] + a_ref[...].astype(F32) + b_ref[...].astype(F32) + c_ref[...].astype(F32)
    out_ref[...] = total.T.astype(BF)


def whole(shape, dtype):
    return jax.ShapeDtypeStruct(shape, dtype)


VM = pl.BlockSpec(memory_space=pltpu.VMEM)
ANY = pl.BlockSpec(memory_space=pl.ANY)
HB = pl.BlockSpec(memory_space=pltpu.HBM)


def layer(
    query_act, key_act, value_act, attn_out, out_grad, log_sum, positions, w_query, w_key, w_value
):
    pack, kv, mark = pl.pallas_call(
        prep_kernel,
        out_shape=(
            whole((2 * PIECE, 1024), BF),
            whole((ROWS + 16, 256), BF),
            whole((8, 128), F32),
        ),
        in_specs=[HB] * 7,
        out_specs=(VM, VM, VM),
        scratch_shapes=[
            pltpu.SMEM((ROWS,), jnp.int32),
            pltpu.VMEM((ROWS, 512), BF),
            pltpu.VMEM((REPEAT, ROWS), F32),
            pltpu.SemaphoreType.DMA((9,)),
        ],
        compiler_params=pltpu.CompilerParams(vmem_limit_bytes=PREP_LIMIT),
    )(positions, query_act, out_grad, attn_out, log_sum, key_act, value_act)

    mark = pl.pallas_call(
        pause_kernel,
        out_shape=whole((8, 128), F32),
        in_specs=[ANY],
        out_specs=ANY,
        cost_estimate=pl.CostEstimate(flops=8_000_000_000, bytes_accessed=8192, transcendentals=0),
    )(mark)

    left = move_y(pack, 1)
    right = move_y(pack, -1)
    up1 = move_z(kv, 1)
    down1 = move_z(kv, -1)
    up2 = move_z(kv, 2)
    down2 = move_z(kv, -2)
    up3 = move_z(up2, 1)
    down3 = move_z(down2, -1)
    up4 = move_z(up2, 2)
    far0 = move_y(left[0:PIECE], 1)
    far1 = move_y(right[PIECE : 2 * PIECE], -1)

    near = [kv, up1, down1, up2, down2]
    first = attend([pack, left, right], near, [None] * 3, [None] * 5, [F32] * 3, [F32] * 5)
    outer = attend(
        [pack, left, right, far0, far1],
        [up3, down3, up4],
        list(first[0:3]) + [None],
        [None] * 3,
        [F32, BF, BF, F32],
        [BF] * 2,
        ((0, 1, 4), (2, 3, 5)),
    )
    back_up = move_z(outer[4], -2)
    back_down = move_z(outer[5], 2)
    last = attend([far0, far1], near, [outer[3]], list(first[3:8]), [BF], [F32] * 5)
    dqs = [outer[0], move_y(outer[1], -1), move_y(outer[2], 1), move_y(last[0], 2)]
    merged = pl.pallas_call(
        merge_kernel,
        out_shape=(whole((ROWS, 256), BF),) * 4,
        in_specs=[VM] * 6,
        out_specs=(VM,) * 4,
        compiler_params=pltpu.CompilerParams(vmem_limit_bytes=8 * MIB),
    )(*last[2:6], back_up, back_down)
    dkvs = [last[1]] + [move_z(merged[i], steps) for i, steps in ((2, -2), (3, 2), (0, -1), (1, 1))]

    freqs = 500000.0 ** (-(jnp.arange(HALF, dtype=F32) * 2.0 / HEAD_DIM))
    angles = freqs[:, None] * positions.astype(F32)[None, :]
    cosine = jnp.cos(angles)
    sine = jnp.sin(angles)

    grads, to_send = pl.pallas_call(
        send_kernel,
        out_shape=(whole((768, ROWS), BF), whole((NX, 512, ROWS), BF)),
        in_specs=[VM] * 14 + [ANY],
        out_specs=(VM, VM),
        compiler_params=pltpu.CompilerParams(vmem_limit_bytes=20 * MIB),
    )(*dqs, *dkvs, cosine, sine, w_query, w_key, w_value, mark)
    got = swap_core(to_send)
    kept = pl.pallas_call(
        keep_kernel,
        out_shape=whole((NX, 512, ROWS), F32),
        in_specs=[VM] * 4,
        out_specs=VM,
        compiler_params=pltpu.CompilerParams(vmem_limit_bytes=20 * MIB),
        cost_estimate=pl.CostEstimate(
            flops=800_000_000, bytes_accessed=4_000_000, transcendentals=0
        ),
    )(grads, w_query, w_key, w_value)
    parts = [kept[i] + got[i].astype(F32) for i in range(4)]
    came = [move_x(parts[i].astype(BF), i) for i in (2, 1, 3)]
    return pl.pallas_call(
        final_kernel,
        out_shape=whole((ROWS, 512), BF),
        in_specs=[VM] * 4,
        out_specs=VM,
        compiler_params=pltpu.CompilerParams(vmem_limit_bytes=8 * MIB),
    )(parts[0], *came)


def solution(mesh):
    return jax.shard_map(
        layer,
        mesh=mesh,
        in_specs=(
            P("seq", "tp"),
            P("seq", "tp"),
            P("seq", "tp"),
            P("seq", "tp"),
            P("seq", "tp"),
            P("tp", "seq"),
            P("seq"),
            P(None, "tp"),
            P(None, "tp"),
            P(None, "tp"),
        ),
        out_specs=P("seq", "tp"),
        check_vma=False,
    )
```

```python
import functools

import jax
import jax.numpy as jnp
from jax import lax
from jax.experimental import pallas as pl
from jax.experimental.pallas import tpu as pltpu
from jax.sharding import PartitionSpec as P


HEADS = 32
KV_HEADS = 8
HEAD_DIM = 128
REPEAT = HEADS // KV_HEADS
HALF = HEAD_DIM // 2
CHUNK = 128
ROWS = 256
NZ, NY, NX, NC = 8, 4, 4, 2
LOG2E = 1.4426950408889634
SCALE = HEAD_DIM**-0.5
BF = jnp.bfloat16
F32 = jnp.float32
PIECE = CHUNK + 16
UNROLL = 2
MIB = 1024 * 1024
PREP_LIMIT = 63 * MIB


def dot(a, b, dims, precision=None):
    return lax.dot_general(
        a, b, (dims, ((), ())), preferred_element_type=F32, precision=precision
    )


NN = ((1,), (0,))
NT = ((1,), (1,))


def move_z(value, steps):
    pairs = [
        (z * NY + y, ((z + steps) % NZ) * NY + y) for z in range(NZ) for y in range(NY)
    ]
    return lax.ppermute(value, "seq", pairs)


def move_y(value, steps):
    pairs = [
        (z * NY + y, z * NY + (y + steps) % NY) for z in range(NZ) for y in range(NY)
    ]
    return lax.ppermute(value, "seq", pairs)


def move_x(value, steps):
    pairs = [
        (x * NC + c, ((x + steps) % NX) * NC + c) for x in range(NX) for c in range(NC)
    ]
    return lax.ppermute(value, "tp", pairs)


def swap_core(value):
    pairs = [(x * NC + c, x * NC + 1 - c) for x in range(NX) for c in range(NC)]
    return lax.ppermute(value, "tp", pairs)


def split3(value):
    high = value.astype(BF)
    rest = value - high.astype(F32)
    mid = rest.astype(BF)
    low = (rest - mid.astype(F32)).astype(BF)
    return high, mid, low


def prep_kernel(
    pos_hbm, q_hbm, do_hbm, o_hbm, lse_hbm, k_hbm, v_hbm, pack_ref, kv_ref, mark_ref, *scratch
):
    mark_ref[...] = jnp.zeros_like(mark_ref)
    pos_ref, o_ref, lse_ref, sems = scratch
    copies = [
        pltpu.make_async_copy(pos_hbm, pos_ref, sems.at[0]),
        pltpu.make_async_copy(lse_hbm, lse_ref, sems.at[1]),
        pltpu.make_async_copy(o_hbm, o_ref, sems.at[2]),
        pltpu.make_async_copy(k_hbm, kv_ref.at[0:ROWS, 0:128], sems.at[3]),
        pltpu.make_async_copy(v_hbm, kv_ref.at[0:ROWS, 128:256], sems.at[4]),
    ]
    for c in range(2):
        rows = slice(c * CHUNK, c * CHUNK + CHUNK)
        into = slice(c * PIECE, c * PIECE + CHUNK)
        copies.append(
            pltpu.make_async_copy(do_hbm.at[rows], pack_ref.at[into, 512:1024], sems.at[5 + c])
        )
        copies.append(
            pltpu.make_async_copy(q_hbm.at[rows], pack_ref.at[into, 0:512], sems.at[7 + c])
        )
    for copy in copies:
        copy.start()
    for copy in copies:
        copy.wait()
    ones = jnp.ones((8, HEAD_DIM), F32)
    index = lax.broadcasted_iota(jnp.int32, (16, 256), 0)
    first = (pos_ref[0] // CHUNK).astype(F32)
    second = (pos_ref[CHUNK] // CHUNK).astype(F32)
    kv_ref[ROWS : ROWS + 16, :] = jnp.where(index == 0, first, second).astype(BF)
    for c in range(2):
        base = c * PIECE
        rows = slice(c * CHUNK, c * CHUNK + CHUNK)
        deltas = []
        for h in range(REPEAT):
            dout = pack_ref[base : base + CHUNK, 512 + h * 128 : 640 + h * 128].astype(F32)
            prod = dout * o_ref[rows, h * 128 : h * 128 + 128].astype(F32)
            deltas.append(dot(ones, prod, NT, lax.Precision.HIGHEST)[0:1])
        lse_row = jnp.concatenate([lse_ref[h : h + 1, rows] for h in range(REPEAT)], axis=1)
        delta_row = jnp.concatenate(deltas, axis=1)
        row = jnp.concatenate([lse_row * LOG2E, delta_row * SCALE], axis=1)
        parts = [part.astype(F32) for part in split3(row)]
        parts.append(jnp.full((1, 1024), second if c else first, F32))
        block = jnp.concatenate(parts + [jnp.zeros((12, 1024), F32)], axis=0)
        pack_ref[base + CHUNK : base + PIECE, :] = block.astype(BF)


def pause_kernel(mark_ref, out_ref):
    del mark_ref, out_ref


def attn_kernel(q_sizes, nkv, has_dq, has_dkv, layout, *refs):
    refs = list(refs)

    def take(count):
        out = refs[:count]
        del refs[:count]
        return out

    packs = take(len(q_sizes))
    kvs = take(nkv)
    dq_ins = take(sum(has_dq))
    dkv_ins = take(sum(has_dkv))
    nblocks = sum(q_sizes) // 2
    dq_outs = take(nblocks)
    dkv_outs = take(len(layout))
    qc, doc, ks, vs, kts, rowc, dq_acc, dk_acc, dv_acc, qst, kst, ln, lc, lg = refs
    nq = 2 * nblocks
    nk = 2 * nkv

    n = 0
    for ref, size in zip(packs, q_sizes):
        for c in range(size):
            base = c * PIECE
            meta = ref[base + CHUNK : base + PIECE, :].astype(F32)
            row = meta[0:1] + meta[1:2] + meta[2:3]
            rowc[n] = jnp.broadcast_to(row, (8, 1024))
            qst[n] = jnp.max(meta[3:4, 0:128]).astype(jnp.int32)
            for h in range(REPEAT):
                rows = slice(h * 128, h * 128 + 128)
                qc[n, rows, :] = ref[base : base + CHUNK, h * 128 : h * 128 + 128]
                doc[n, rows, :] = ref[base : base + CHUNK, 512 + h * 128 : 640 + h * 128]
            n += 1
    for j in range(nkv):
        meta = kvs[j][ROWS : ROWS + 16, :].astype(F32)
        for c in range(2):
            rows = slice(c * 128, c * 128 + 128)
            kst[2 * j + c] = jnp.max(meta[c : c + 1, 0:128]).astype(jnp.int32)
            ks[2 * j + c] = kvs[j][rows, 0:128]
            vs[2 * j + c] = kvs[j][rows, 128:256]
            kts[2 * j + c] = kvs[j][rows, 0:128].T
    at = 0
    for b in range(nblocks):
        for c in range(2):
            for h in range(REPEAT):
                lanes = slice(h * 128, h * 128 + 128)
                if has_dq[b]:
                    dq_acc[2 * b + c, :, lanes] = dq_ins[at][lanes, c * 128 : c * 128 + 128]
                else:
                    dq_acc[2 * b + c, :, lanes] = jnp.zeros((128, 128), F32)
        at += has_dq[b]
    at = 0
    for j in range(nkv):
        for c in range(2):
            rows = slice(c * 128, c * 128 + 128)
            if has_dkv[j]:
                dk_acc[2 * j + c] = dkv_ins[at][rows, 0:128]
                dv_acc[2 * j + c] = dkv_ins[at][rows, 128:256]
            else:
                dk_acc[2 * j + c] = jnp.zeros((128, 128), F32)
                dv_acc[2 * j + c] = jnp.zeros((128, 128), F32)
        at += has_dkv[j]

    def per_query(n, count):
        place = qst[n]
        for c in range(nk):
            gap = (place - kst[c]) * CHUNK
            ln[count] = n
            lc[count] = c
            lg[count] = gap
            count = count + (gap >= 0).astype(jnp.int32)
        ln[count] = n
        lc[count] = 0
        lg[count] = -100000
        return count + (count & 1)

    count = lax.fori_loop(0, nq, per_query, jnp.int32(0))
    for extra in range(2 * UNROLL - 2):
        ln[count + extra] = 0
        lc[count + extra] = 0
        lg[count + extra] = -100000

    line = lax.broadcasted_iota(jnp.int32, (128, 256), 0)
    lane = lax.broadcasted_iota(jnp.int32, (128, 256), 1) & 127
    diff = line - lane

    def load(t):
        n, c1, c2 = ln[2 * t], lc[2 * t], lc[2 * t + 1]
        k = jnp.concatenate([ks[c1], ks[c2]], axis=0)
        v = jnp.concatenate([vs[c1], vs[c2]], axis=0)
        return n, c1, c2, k, v, (lg[2 * t], lg[2 * t + 1])

    def opening(unit):
        (n, _, _, k, v, _), half = unit
        lanes = slice(half * 256, half * 256 + 256)
        return dot(k, qc[n, lanes, :], NT), dot(v, doc[n, lanes, :], NT)

    def middle(unit, found):
        (n, _, _, _, _, mask), half = unit
        scores = found[0] * (SCALE * LOG2E) - rowc[n, 0:1, half * 256 : half * 256 + 256]
        probs = jnp.exp2(scores)
        probs = jnp.concatenate(
            [
                jnp.where(diff <= mask[0], probs[0:128], 0.0),
                jnp.where(diff <= mask[1], probs[128:256], 0.0),
            ],
            axis=0,
        )
        dprob = found[1] * SCALE - rowc[n, 0:1, 512 + half * 256 : 768 + half * 256]
        return probs.astype(BF), (probs * dprob).astype(BF)

    def closing(unit, made, sums):
        (n, c1, c2, _, _, _), half = unit
        lanes = slice(half * 256, half * 256 + 256)
        probs, dscore = made
        dv = dot(probs, doc[n, lanes, :], NN)
        dk = dot(dscore, qc[n, lanes, :], NN)
        kt = jnp.concatenate([kts[c1], kts[c2]], axis=1)
        dq_acc[n, :, lanes] += dot(kt, dscore, NN)
        if half == 0:
            return dk, dv
        dk = dk + sums[0]
        dv = dv + sums[1]
        dk_acc[c1] += dk[0:128]
        dv_acc[c1] += dv[0:128]
        dk_acc[c2] += dk[128:256]
        dv_acc[c2] += dv[128:256]
        return None

    def turn(i, carry):
        units = []
        for step in range(UNROLL):
            info = load(i * UNROLL + step)
            units += [(info, 0), (info, 1)]
        found = {0: opening(units[0])}
        sums = None
        made = {}
        for at in range(len(units) + 1):
            if at + 1 < len(units):
                found[at + 1] = opening(units[at + 1])
            if at < len(units):
                made[at] = middle(units[at], found.pop(at))
            if at >= 1:
                sums = closing(units[at - 1], made.pop(at - 1), sums)
        return carry

    lax.fori_loop(0, (count + 2 * UNROLL - 1) // (2 * UNROLL), turn, 0)

    for b in range(nblocks):
        for c in range(2):
            for h in range(REPEAT):
                rows = slice(h * 128, h * 128 + 128)
                dq_outs[b][rows, c * 128 : c * 128 + 128] = dq_acc[2 * b + c, :, rows].astype(
                    dq_outs[b].dtype
                )
    for ref, held in zip(dkv_outs, layout):
        for at, c in enumerate(held):
            rows = slice(at * 128, at * 128 + 128)
            ref[rows, 0:128] = dk_acc[c].astype(ref.dtype)
            ref[rows, 128:256] = dv_acc[c].astype(ref.dtype)


def attend(packs, kvs, dq_ins, dkv_ins, dq_types, dkv_types, layout=None):
    layout = layout or tuple((2 * j, 2 * j + 1) for j in range(len(kvs)))
    sizes = tuple(p.shape[0] // PIECE for p in packs)
    nq = sum(sizes)
    nk = 2 * len(kvs)
    has_dq = tuple(int(g is not None) for g in dq_ins)
    has_dkv = tuple(int(g is not None) for g in dkv_ins)
    operands = list(packs) + list(kvs) + [g for g in list(dq_ins) + list(dkv_ins) if g is not None]
    most = nq * (nk + 1) + 2 * UNROLL
    return pl.pallas_call(
        functools.partial(attn_kernel, sizes, len(kvs), has_dq, has_dkv, layout),
        out_shape=tuple(whole((512, ROWS), t) for t in dq_types)
        + tuple(whole((128 * len(held), 256), t) for held, t in zip(layout, dkv_types)),
        in_specs=[VM] * len(operands),
        out_specs=(VM,) * (len(dq_types) + len(dkv_types)),
        scratch_shapes=[
            pltpu.VMEM((nq, 512, 128), BF),
            pltpu.VMEM((nq, 512, 128), BF),
            pltpu.VMEM((nk, 128, 128), BF),
            pltpu.VMEM((nk, 128, 128), BF),
            pltpu.VMEM((nk, 128, 128), BF),
            pltpu.VMEM((nq, 8, 1024), F32),
            pltpu.VMEM((nq, 128, 512), F32),
            pltpu.VMEM((nk, 128, 128), F32),
            pltpu.VMEM((nk, 128, 128), F32),
            pltpu.SMEM((nq,), jnp.int32),
            pltpu.SMEM((nk,), jnp.int32),
        ]
        + [pltpu.SMEM((most,), jnp.int32)] * 3,
        compiler_params=pltpu.CompilerParams(vmem_limit_bytes=28 * MIB),
        cost_estimate=pl.CostEstimate(
            flops=nq * nk * 85_000_000, bytes_accessed=4_000_000, transcendentals=nq * nk * 65536
        ),
    )(*operands)


def rotate(value, cosine, sine):
    first = value[0:HALF]
    second = value[HALF : 2 * HALF]
    return jnp.concatenate(
        [first * cosine + second * sine, second * cosine - first * sine], axis=0
    )


def block_rows(i):
    tp = lax.axis_index("tp")
    core = tp % NC
    block = NC * lax.rem(tp // NC + i % NX, NX) + (1 - core if i < NX else core)
    return pl.ds(pl.multiple_of(block * 512, 512), 512)


def query_kernel(*refs):
    dqs = refs[0:4]
    cos_ref, sin_ref, wq_ref, out_ref, x_ref = refs[4:]
    cosine = cos_ref[...]
    sine = sin_ref[...]
    for head in range(REPEAT):
        rows = slice(head * 128, head * 128 + 128)
        total = dqs[0][rows, :]
        for ref in dqs[1:]:
            total = total + ref[rows, :].astype(F32)
        x_ref[rows, :] = rotate(total, cosine, sine).astype(BF)
    for i in range(2 * NX):
        out_ref[i] = dot(wq_ref[block_rows(i), :], x_ref[...], NN)


def add_terms(part_ref, x_ref, wk_ref, wv_ref, i):
    rows = block_rows(i)
    return (
        part_ref[i]
        + dot(wk_ref[rows, :], x_ref[0:128, :], NN)
        + dot(wv_ref[rows, :], x_ref[128:256, :], NN)
    )


def send_kernel(*refs):
    dkvs = refs[0:5]
    cos_ref, sin_ref, part_ref, wk_ref, wv_ref, _, x_out, out_ref = refs[5:]
    total = dkvs[0][...]
    for ref in dkvs[1:]:
        total = total + ref[...].astype(F32)
    x_out[0:128, :] = rotate(total[:, 0:128].T, cos_ref[...], sin_ref[...]).astype(BF)
    x_out[128:256, :] = total[:, 128:256].T.astype(BF)
    for i in range(NX):
        out_ref[i] = add_terms(part_ref, x_out, wk_ref, wv_ref, i).astype(BF)


def keep_kernel(x_ref, part_ref, wk_ref, wv_ref, out_ref):
    for i in range(NX):
        out_ref[i] = add_terms(part_ref, x_ref, wk_ref, wv_ref, NX + i)


def merge_kernel(up1, down1, up2, down2, from_up, from_down, *outs):
    outs[0][...] = (up1[...] + from_up[0:256, :].astype(F32)).astype(BF)
    outs[1][...] = (down1[...] + from_down[0:256, :].astype(F32)).astype(BF)
    outs[2][0:128, :] = (up2[0:128, :] + from_up[256:384, :].astype(F32)).astype(BF)
    outs[2][128:256, :] = up2[128:256, :].astype(BF)
    outs[3][0:128, :] = down2[0:128, :].astype(BF)
    outs[3][128:256, :] = (down2[128:256, :] + from_down[256:384, :].astype(F32)).astype(BF)


def final_kernel(own_ref, a_ref, b_ref, c_ref, out_ref):
    total = own_ref[...] + a_ref[...].astype(F32) + b_ref[...].astype(F32) + c_ref[...].astype(F32)
    out_ref[...] = total.T.astype(BF)


def whole(shape, dtype):
    return jax.ShapeDtypeStruct(shape, dtype)


VM = pl.BlockSpec(memory_space=pltpu.VMEM)
ANY = pl.BlockSpec(memory_space=pl.ANY)
HB = pl.BlockSpec(memory_space=pltpu.HBM)


def layer(
    query_act, key_act, value_act, attn_out, out_grad, log_sum, positions, w_query, w_key, w_value
):
    pack, kv, mark = pl.pallas_call(
        prep_kernel,
        out_shape=(
            whole((2 * PIECE, 1024), BF),
            whole((ROWS + 16, 256), BF),
            whole((8, 128), F32),
        ),
        in_specs=[HB] * 7,
        out_specs=(VM, VM, VM),
        scratch_shapes=[
            pltpu.SMEM((ROWS,), jnp.int32),
            pltpu.VMEM((ROWS, 512), BF),
            pltpu.VMEM((REPEAT, ROWS), F32),
            pltpu.SemaphoreType.DMA((9,)),
        ],
        compiler_params=pltpu.CompilerParams(vmem_limit_bytes=PREP_LIMIT),
    )(positions, query_act, out_grad, attn_out, log_sum, key_act, value_act)

    mark = pl.pallas_call(
        pause_kernel,
        out_shape=whole((8, 128), F32),
        in_specs=[ANY],
        out_specs=ANY,
        cost_estimate=pl.CostEstimate(flops=8_000_000_000, bytes_accessed=8192, transcendentals=0),
    )(mark)

    left = move_y(pack, 1)
    right = move_y(pack, -1)
    up1 = move_z(kv, 1)
    down1 = move_z(kv, -1)
    up2 = move_z(kv, 2)
    down2 = move_z(kv, -2)
    up3 = move_z(up2, 1)
    down3 = move_z(down2, -1)
    up4 = move_z(up2, 2)
    far0 = move_y(left[0:PIECE], 1)
    far1 = move_y(right[PIECE : 2 * PIECE], -1)

    near = [kv, up1, down1, up2, down2]
    first = attend([pack, left, right], near, [None] * 3, [None] * 5, [F32] * 3, [F32] * 5)
    outer = attend(
        [pack, left, right, far0, far1],
        [up3, down3, up4],
        list(first[0:3]) + [None],
        [None] * 3,
        [F32, BF, BF, F32],
        [BF] * 2,
        ((0, 1, 4), (2, 3, 5)),
    )
    back_up = move_z(outer[4], -2)
    back_down = move_z(outer[5], 2)
    last = attend([far0, far1], near, [outer[3]], list(first[3:8]), [BF], [F32] * 5)
    dqs = [outer[0], move_y(outer[1], -1), move_y(outer[2], 1), move_y(last[0], 2)]
    merged = pl.pallas_call(
        merge_kernel,
        out_shape=(whole((ROWS, 256), BF),) * 4,
        in_specs=[VM] * 6,
        out_specs=(VM,) * 4,
        compiler_params=pltpu.CompilerParams(vmem_limit_bytes=8 * MIB),
    )(*last[2:6], back_up, back_down)
    dkvs = [last[1]] + [move_z(merged[i], steps) for i, steps in ((2, -2), (3, 2), (0, -1), (1, 1))]

    freqs = 500000.0 ** (-(jnp.arange(HALF, dtype=F32) * 2.0 / HEAD_DIM))
    angles = freqs[:, None] * positions.astype(F32)[None, :]
    cosine = jnp.cos(angles)
    sine = jnp.sin(angles)

    part = pl.pallas_call(
        query_kernel,
        out_shape=whole((2 * NX, 512, ROWS), F32),
        in_specs=[VM] * 7,
        out_specs=VM,
        scratch_shapes=[pltpu.VMEM((512, ROWS), BF)],
        compiler_params=pltpu.CompilerParams(vmem_limit_bytes=20 * MIB),
        cost_estimate=pl.CostEstimate(
            flops=1_100_000_000, bytes_accessed=8_000_000, transcendentals=0
        ),
    )(*dqs, cosine, sine, w_query)
    grads, to_send = pl.pallas_call(
        send_kernel,
        out_shape=(whole((256, ROWS), BF), whole((NX, 512, ROWS), BF)),
        in_specs=[VM] * 10 + [ANY],
        out_specs=(VM, VM),
        compiler_params=pltpu.CompilerParams(vmem_limit_bytes=20 * MIB),
    )(*dkvs, cosine, sine, part, w_key, w_value, mark)
    got = swap_core(to_send)
    kept = pl.pallas_call(
        keep_kernel,
        out_shape=whole((NX, 512, ROWS), F32),
        in_specs=[VM] * 4,
        out_specs=VM,
        compiler_params=pltpu.CompilerParams(vmem_limit_bytes=20 * MIB),
        cost_estimate=pl.CostEstimate(
            flops=800_000_000, bytes_accessed=4_000_000, transcendentals=0
        ),
    )(grads, part, w_key, w_value)
    parts = [kept[i] + got[i].astype(F32) for i in range(4)]
    came = [move_x(parts[i].astype(BF), i) for i in (2, 1, 3)]
    return pl.pallas_call(
        final_kernel,
        out_shape=whole((ROWS, 512), BF),
        in_specs=[VM] * 4,
        out_specs=VM,
        compiler_params=pltpu.CompilerParams(vmem_limit_bytes=8 * MIB),
    )(parts[0], *came)


def solution(mesh):
    return jax.shard_map(
        layer,
        mesh=mesh,
        in_specs=(
            P("seq", "tp"),
            P("seq", "tp"),
            P("seq", "tp"),
            P("seq", "tp"),
            P("seq", "tp"),
            P("tp", "seq"),
            P("seq"),
            P(None, "tp"),
            P(None, "tp"),
            P(None, "tp"),
        ),
        out_specs=P("seq", "tp"),
        check_vma=False,
    )
```

```python
import functools

import jax
import jax.numpy as jnp
from jax import lax
from jax.experimental import pallas as pl
from jax.experimental.pallas import tpu as pltpu
from jax.sharding import PartitionSpec as P


HEADS = 32
KV_HEADS = 8
HEAD_DIM = 128
REPEAT = HEADS // KV_HEADS
HALF = HEAD_DIM // 2
CHUNK = 128
ROWS = 256
NZ, NY, NX, NC = 8, 4, 4, 2
LOG2E = 1.4426950408889634
SCALE = HEAD_DIM**-0.5
BF = jnp.bfloat16
F32 = jnp.float32
PIECE = CHUNK + 16
UNROLL = 2
MIB = 1024 * 1024
PREP_LIMIT = 63 * MIB


def dot(a, b, dims, precision=None):
    return lax.dot_general(
        a, b, (dims, ((), ())), preferred_element_type=F32, precision=precision
    )


NN = ((1,), (0,))
NT = ((1,), (1,))


def move_z(value, steps):
    pairs = [
        (z * NY + y, ((z + steps) % NZ) * NY + y) for z in range(NZ) for y in range(NY)
    ]
    return lax.ppermute(value, "seq", pairs)


def move_y(value, steps):
    pairs = [
        (z * NY + y, z * NY + (y + steps) % NY) for z in range(NZ) for y in range(NY)
    ]
    return lax.ppermute(value, "seq", pairs)


def move_x(value, steps):
    pairs = [
        (x * NC + c, ((x + steps) % NX) * NC + c) for x in range(NX) for c in range(NC)
    ]
    return lax.ppermute(value, "tp", pairs)


def swap_core(value):
    pairs = [(x * NC + c, x * NC + 1 - c) for x in range(NX) for c in range(NC)]
    return lax.ppermute(value, "tp", pairs)


def split3(value):
    high = value.astype(BF)
    rest = value - high.astype(F32)
    mid = rest.astype(BF)
    low = (rest - mid.astype(F32)).astype(BF)
    return high, mid, low


def prep_kernel(
    pos_hbm, q_hbm, do_hbm, o_hbm, lse_hbm, k_hbm, v_hbm, pack_ref, kv_ref, mark_ref, *scratch
):
    mark_ref[...] = jnp.zeros_like(mark_ref)
    pos_ref, o_ref, lse_ref, sems = scratch
    copies = [
        pltpu.make_async_copy(pos_hbm, pos_ref, sems.at[0]),
        pltpu.make_async_copy(lse_hbm, lse_ref, sems.at[1]),
        pltpu.make_async_copy(o_hbm, o_ref, sems.at[2]),
        pltpu.make_async_copy(k_hbm, kv_ref.at[0:ROWS, 0:128], sems.at[3]),
        pltpu.make_async_copy(v_hbm, kv_ref.at[0:ROWS, 128:256], sems.at[4]),
    ]
    for c in range(2):
        rows = slice(c * CHUNK, c * CHUNK + CHUNK)
        into = slice(c * PIECE, c * PIECE + CHUNK)
        copies.append(
            pltpu.make_async_copy(do_hbm.at[rows], pack_ref.at[into, 512:1024], sems.at[5 + c])
        )
        copies.append(
            pltpu.make_async_copy(q_hbm.at[rows], pack_ref.at[into, 0:512], sems.at[7 + c])
        )
    for copy in copies:
        copy.start()
    for copy in copies:
        copy.wait()
    ones = jnp.ones((8, HEAD_DIM), F32)
    index = lax.broadcasted_iota(jnp.int32, (16, 256), 0)
    first = (pos_ref[0] // CHUNK).astype(F32)
    second = (pos_ref[CHUNK] // CHUNK).astype(F32)
    kv_ref[ROWS : ROWS + 16, :] = jnp.where(index == 0, first, second).astype(BF)
    for c in range(2):
        base = c * PIECE
        rows = slice(c * CHUNK, c * CHUNK + CHUNK)
        deltas = []
        for h in range(REPEAT):
            dout = pack_ref[base : base + CHUNK, 512 + h * 128 : 640 + h * 128].astype(F32)
            prod = dout * o_ref[rows, h * 128 : h * 128 + 128].astype(F32)
            deltas.append(dot(ones, prod, NT, lax.Precision.HIGHEST)[0:1])
        lse_row = jnp.concatenate([lse_ref[h : h + 1, rows] for h in range(REPEAT)], axis=1)
        delta_row = jnp.concatenate(deltas, axis=1)
        row = jnp.concatenate([lse_row * LOG2E, delta_row * SCALE], axis=1)
        parts = [part.astype(F32) for part in split3(row)]
        parts.append(jnp.full((1, 1024), second if c else first, F32))
        block = jnp.concatenate(parts + [jnp.zeros((12, 1024), F32)], axis=0)
        pack_ref[base + CHUNK : base + PIECE, :] = block.astype(BF)


def pause_kernel(mark_ref, out_ref):
    del mark_ref, out_ref


def attn_kernel(q_sizes, nkv, has_dq, has_dkv, layout, *refs):
    refs = list(refs)

    def take(count):
        out = refs[:count]
        del refs[:count]
        return out

    packs = take(len(q_sizes))
    kvs = take(nkv)
    dq_ins = take(sum(has_dq))
    dkv_ins = take(sum(has_dkv))
    nblocks = sum(q_sizes) // 2
    dq_outs = take(nblocks)
    dkv_outs = take(len(layout))
    qc, doc, ks, vs, kts, rowc, dq_acc, dk_acc, dv_acc, qst, kst, ln, lc, lg = refs
    nq = 2 * nblocks
    nk = 2 * nkv

    n = 0
    for ref, size in zip(packs, q_sizes):
        for c in range(size):
            base = c * PIECE
            meta = ref[base + CHUNK : base + PIECE, :].astype(F32)
            row = meta[0:1] + meta[1:2] + meta[2:3]
            rowc[n] = jnp.broadcast_to(row, (8, 1024))
            qst[n] = jnp.max(meta[3:4, 0:128]).astype(jnp.int32)
            for h in range(REPEAT):
                rows = slice(h * 128, h * 128 + 128)
                qc[n, rows, :] = ref[base : base + CHUNK, h * 128 : h * 128 + 128]
                doc[n, rows, :] = ref[base : base + CHUNK, 512 + h * 128 : 640 + h * 128]
            n += 1
    for j in range(nkv):
        meta = kvs[j][ROWS : ROWS + 16, :].astype(F32)
        for c in range(2):
            rows = slice(c * 128, c * 128 + 128)
            kst[2 * j + c] = jnp.max(meta[c : c + 1, 0:128]).astype(jnp.int32)
            ks[2 * j + c] = kvs[j][rows, 0:128]
            vs[2 * j + c] = kvs[j][rows, 128:256]
            kts[2 * j + c] = kvs[j][rows, 0:128].T
    at = 0
    for b in range(nblocks):
        for c in range(2):
            for h in range(REPEAT):
                lanes = slice(h * 128, h * 128 + 128)
                if has_dq[b]:
                    dq_acc[2 * b + c, :, lanes] = dq_ins[at][lanes, c * 128 : c * 128 + 128]
                else:
                    dq_acc[2 * b + c, :, lanes] = jnp.zeros((128, 128), F32)
        at += has_dq[b]
    at = 0
    for j in range(nkv):
        for c in range(2):
            rows = slice(c * 128, c * 128 + 128)
            if has_dkv[j]:
                dk_acc[2 * j + c] = dkv_ins[at][rows, 0:128]
                dv_acc[2 * j + c] = dkv_ins[at][rows, 128:256]
            else:
                dk_acc[2 * j + c] = jnp.zeros((128, 128), F32)
                dv_acc[2 * j + c] = jnp.zeros((128, 128), F32)
        at += has_dkv[j]

    def per_query(n, count):
        place = qst[n]
        for c in range(nk):
            gap = (place - kst[c]) * CHUNK
            ln[count] = n
            lc[count] = c
            lg[count] = gap
            count = count + (gap >= 0).astype(jnp.int32)
        ln[count] = n
        lc[count] = 0
        lg[count] = -100000
        return count + (count & 1)

    count = lax.fori_loop(0, nq, per_query, jnp.int32(0))
    for extra in range(2 * UNROLL - 2):
        ln[count + extra] = 0
        lc[count + extra] = 0
        lg[count + extra] = -100000

    line = lax.broadcasted_iota(jnp.int32, (128, 256), 0)
    lane = lax.broadcasted_iota(jnp.int32, (128, 256), 1) & 127
    diff = line - lane

    def load(t):
        n, c1, c2 = ln[2 * t], lc[2 * t], lc[2 * t + 1]
        k = jnp.concatenate([ks[c1], ks[c2]], axis=0)
        v = jnp.concatenate([vs[c1], vs[c2]], axis=0)
        return n, c1, c2, k, v, (lg[2 * t], lg[2 * t + 1])

    def opening(unit):
        (n, _, _, k, v, _), half = unit
        lanes = slice(half * 256, half * 256 + 256)
        return dot(k, qc[n, lanes, :], NT), dot(v, doc[n, lanes, :], NT)

    def middle(unit, found):
        (n, _, _, _, _, mask), half = unit
        scores = found[0] * (SCALE * LOG2E) - rowc[n, 0:1, half * 256 : half * 256 + 256]
        probs = jnp.exp2(scores)
        probs = jnp.concatenate(
            [
                jnp.where(diff <= mask[0], probs[0:128], 0.0),
                jnp.where(diff <= mask[1], probs[128:256], 0.0),
            ],
            axis=0,
        )
        dprob = found[1] * SCALE - rowc[n, 0:1, 512 + half * 256 : 768 + half * 256]
        return probs.astype(BF), (probs * dprob).astype(BF)

    def closing(unit, made, sums):
        (n, c1, c2, _, _, _), half = unit
        lanes = slice(half * 256, half * 256 + 256)
        probs, dscore = made
        dv = dot(probs, doc[n, lanes, :], NN)
        dk = dot(dscore, qc[n, lanes, :], NN)
        kt = jnp.concatenate([kts[c1], kts[c2]], axis=1)
        dq_acc[n, :, lanes] += dot(kt, dscore, NN)
        if half == 0:
            return dk, dv
        dk = dk + sums[0]
        dv = dv + sums[1]
        dk_acc[c1] += dk[0:128]
        dv_acc[c1] += dv[0:128]
        dk_acc[c2] += dk[128:256]
        dv_acc[c2] += dv[128:256]
        return None

    def turn(i, carry):
        units = []
        for step in range(UNROLL):
            info = load(i * UNROLL + step)
            units += [(info, 0), (info, 1)]
        found = {0: opening(units[0])}
        sums = None
        made = {}
        for at in range(len(units) + 1):
            if at + 1 < len(units):
                found[at + 1] = opening(units[at + 1])
            if at < len(units):
                made[at] = middle(units[at], found.pop(at))
            if at >= 1:
                sums = closing(units[at - 1], made.pop(at - 1), sums)
        return carry

    lax.fori_loop(0, (count + 2 * UNROLL - 1) // (2 * UNROLL), turn, 0)

    for b in range(nblocks):
        for c in range(2):
            for h in range(REPEAT):
                rows = slice(h * 128, h * 128 + 128)
                dq_outs[b][rows, c * 128 : c * 128 + 128] = dq_acc[2 * b + c, :, rows].astype(
                    dq_outs[b].dtype
                )
    for ref, held in zip(dkv_outs, layout):
        for at, c in enumerate(held):
            rows = slice(at * 128, at * 128 + 128)
            ref[rows, 0:128] = dk_acc[c].astype(ref.dtype)
            ref[rows, 128:256] = dv_acc[c].astype(ref.dtype)


def attend(packs, kvs, dq_ins, dkv_ins, dq_types, dkv_types, layout=None):
    layout = layout or tuple((2 * j, 2 * j + 1) for j in range(len(kvs)))
    sizes = tuple(p.shape[0] // PIECE for p in packs)
    nq = sum(sizes)
    nk = 2 * len(kvs)
    has_dq = tuple(int(g is not None) for g in dq_ins)
    has_dkv = tuple(int(g is not None) for g in dkv_ins)
    operands = list(packs) + list(kvs) + [g for g in list(dq_ins) + list(dkv_ins) if g is not None]
    most = nq * (nk + 1) + 2 * UNROLL
    return pl.pallas_call(
        functools.partial(attn_kernel, sizes, len(kvs), has_dq, has_dkv, layout),
        out_shape=tuple(whole((512, ROWS), t) for t in dq_types)
        + tuple(whole((128 * len(held), 256), t) for held, t in zip(layout, dkv_types)),
        in_specs=[VM] * len(operands),
        out_specs=(VM,) * (len(dq_types) + len(dkv_types)),
        scratch_shapes=[
            pltpu.VMEM((nq, 512, 128), BF),
            pltpu.VMEM((nq, 512, 128), BF),
            pltpu.VMEM((nk, 128, 128), BF),
            pltpu.VMEM((nk, 128, 128), BF),
            pltpu.VMEM((nk, 128, 128), BF),
            pltpu.VMEM((nq, 8, 1024), F32),
            pltpu.VMEM((nq, 128, 512), F32),
            pltpu.VMEM((nk, 128, 128), F32),
            pltpu.VMEM((nk, 128, 128), F32),
            pltpu.SMEM((nq,), jnp.int32),
            pltpu.SMEM((nk,), jnp.int32),
        ]
        + [pltpu.SMEM((most,), jnp.int32)] * 3,
        compiler_params=pltpu.CompilerParams(vmem_limit_bytes=28 * MIB),
        cost_estimate=pl.CostEstimate(
            flops=nq * nk * 85_000_000, bytes_accessed=4_000_000, transcendentals=nq * nk * 65536
        ),
    )(*operands)


def rotate(value, cosine, sine):
    first = value[0:HALF]
    second = value[HALF : 2 * HALF]
    return jnp.concatenate(
        [first * cosine + second * sine, second * cosine - first * sine], axis=0
    )


def block_rows(i):
    tp = lax.axis_index("tp")
    core = tp % NC
    block = NC * lax.rem(tp // NC + i % NX, NX) + (1 - core if i < NX else core)
    return pl.ds(pl.multiple_of(block * 512, 512), 512)


def query_kernel(*refs):
    dqs = refs[0:4]
    cos_ref, sin_ref, wq_ref, keep_ref, send_ref, x_ref = refs[4:]
    cosine = cos_ref[...]
    sine = sin_ref[...]
    for head in range(REPEAT):
        rows = slice(head * 128, head * 128 + 128)
        total = dqs[0][rows, :]
        for ref in dqs[1:]:
            total = total + ref[rows, :].astype(F32)
        x_ref[rows, :] = rotate(total, cosine, sine).astype(BF)
    for i in range(NX):
        send_ref[i] = dot(wq_ref[block_rows(i), :], x_ref[...], NN).astype(BF)
        keep_ref[i] = dot(wq_ref[block_rows(NX + i), :], x_ref[...], NN)


def key_kernel(*refs):
    dkvs = refs[0:5]
    cos_ref, sin_ref, _, x_out = refs[5:]
    total = dkvs[0][...]
    for ref in dkvs[1:]:
        total = total + ref[...].astype(F32)
    x_out[0:128, :] = rotate(total[:, 0:128].T, cos_ref[...], sin_ref[...]).astype(BF)
    x_out[128:256, :] = total[:, 128:256].T.astype(BF)


def sum_kernel(keep_ref, came_ref, x_ref, x_other_ref, wk_ref, wv_ref, wk_other_ref, wv_other_ref, *outs):
    for i in range(NX):
        rows = block_rows(NX + i)
        total = keep_ref[i] + came_ref[i].astype(F32)
        total = total + dot(wk_ref[rows, :], x_ref[0:128, :], NN)
        total = total + dot(wv_ref[rows, :], x_ref[128:256, :], NN)
        total = total + dot(wk_other_ref[rows, :], x_other_ref[0:128, :], NN)
        total = total + dot(wv_other_ref[rows, :], x_other_ref[128:256, :], NN)
        outs[i][...] = total.astype(outs[i].dtype)


def merge_kernel(up1, down1, up2, down2, from_up, from_down, *outs):
    outs[0][...] = (up1[...] + from_up[0:256, :].astype(F32)).astype(BF)
    outs[1][...] = (down1[...] + from_down[0:256, :].astype(F32)).astype(BF)
    outs[2][0:128, :] = (up2[0:128, :] + from_up[256:384, :].astype(F32)).astype(BF)
    outs[2][128:256, :] = up2[128:256, :].astype(BF)
    outs[3][0:128, :] = down2[0:128, :].astype(BF)
    outs[3][128:256, :] = (down2[128:256, :] + from_down[256:384, :].astype(F32)).astype(BF)


def final_kernel(own_ref, a_ref, b_ref, c_ref, out_ref):
    total = own_ref[...] + a_ref[...].astype(F32) + b_ref[...].astype(F32) + c_ref[...].astype(F32)
    out_ref[...] = total.T.astype(BF)


def whole(shape, dtype):
    return jax.ShapeDtypeStruct(shape, dtype)


VM = pl.BlockSpec(memory_space=pltpu.VMEM)
ANY = pl.BlockSpec(memory_space=pl.ANY)
HB = pl.BlockSpec(memory_space=pltpu.HBM)


def layer(
    query_act, key_act, value_act, attn_out, out_grad, log_sum, positions, w_query, w_key, w_value
):
    pack, kv, mark = pl.pallas_call(
        prep_kernel,
        out_shape=(
            whole((2 * PIECE, 1024), BF),
            whole((ROWS + 16, 256), BF),
            whole((8, 128), F32),
        ),
        in_specs=[HB] * 7,
        out_specs=(VM, VM, VM),
        scratch_shapes=[
            pltpu.SMEM((ROWS,), jnp.int32),
            pltpu.VMEM((ROWS, 512), BF),
            pltpu.VMEM((REPEAT, ROWS), F32),
            pltpu.SemaphoreType.DMA((9,)),
        ],
        compiler_params=pltpu.CompilerParams(vmem_limit_bytes=PREP_LIMIT),
    )(positions, query_act, out_grad, attn_out, log_sum, key_act, value_act)

    mark = pl.pallas_call(
        pause_kernel,
        out_shape=whole((8, 128), F32),
        in_specs=[ANY],
        out_specs=ANY,
        cost_estimate=pl.CostEstimate(flops=8_000_000_000, bytes_accessed=8192, transcendentals=0),
    )(mark)

    key_other = swap_core(w_key)
    value_other = swap_core(w_value)
    left = move_y(pack, 1)
    right = move_y(pack, -1)
    up1 = move_z(kv, 1)
    down1 = move_z(kv, -1)
    up2 = move_z(kv, 2)
    down2 = move_z(kv, -2)
    up3 = move_z(up2, 1)
    down3 = move_z(down2, -1)
    up4 = move_z(up2, 2)
    far0 = move_y(left[0:PIECE], 1)
    far1 = move_y(right[PIECE : 2 * PIECE], -1)

    near = [kv, up1, down1, up2, down2]
    first = attend([pack, left, right], near, [None] * 3, [None] * 5, [F32] * 3, [F32] * 5)
    outer = attend(
        [pack, left, right, far0, far1],
        [up3, down3, up4],
        list(first[0:3]) + [None],
        [None] * 3,
        [F32, BF, BF, F32],
        [BF] * 2,
        ((0, 1, 4), (2, 3, 5)),
    )
    back_up = move_z(outer[4], -2)
    back_down = move_z(outer[5], 2)
    last = attend([far0, far1], near, [outer[3]], list(first[3:8]), [BF], [F32] * 5)
    dqs = [outer[0], move_y(outer[1], -1), move_y(outer[2], 1), move_y(last[0], 2)]
    merged = pl.pallas_call(
        merge_kernel,
        out_shape=(whole((ROWS, 256), BF),) * 4,
        in_specs=[VM] * 6,
        out_specs=(VM,) * 4,
        compiler_params=pltpu.CompilerParams(vmem_limit_bytes=8 * MIB),
    )(*last[2:6], back_up, back_down)
    dkvs = [last[1]] + [move_z(merged[i], steps) for i, steps in ((2, -2), (3, 2), (0, -1), (1, 1))]

    freqs = 500000.0 ** (-(jnp.arange(HALF, dtype=F32) * 2.0 / HEAD_DIM))
    angles = freqs[:, None] * positions.astype(F32)[None, :]
    cosine = jnp.cos(angles)
    sine = jnp.sin(angles)

    kept, to_send = pl.pallas_call(
        query_kernel,
        out_shape=(whole((NX, 512, ROWS), F32), whole((NX, 512, ROWS), BF)),
        in_specs=[VM] * 7,
        out_specs=(VM, VM),
        scratch_shapes=[pltpu.VMEM((512, ROWS), BF)],
        compiler_params=pltpu.CompilerParams(vmem_limit_bytes=20 * MIB),
        cost_estimate=pl.CostEstimate(
            flops=1_100_000_000, bytes_accessed=8_000_000, transcendentals=0
        ),
    )(*dqs, cosine, sine, w_query)
    terms = swap_core(to_send)
    grads = pl.pallas_call(
        key_kernel,
        out_shape=whole((256, ROWS), BF),
        in_specs=[VM] * 7 + [ANY],
        out_specs=VM,
        compiler_params=pltpu.CompilerParams(vmem_limit_bytes=8 * MIB),
    )(*dkvs, cosine, sine, mark)
    others = swap_core(grads)
    parts = pl.pallas_call(
        sum_kernel,
        out_shape=(whole((512, ROWS), F32),) + (whole((512, ROWS), BF),) * (NX - 1),
        in_specs=[VM] * 8,
        out_specs=(VM,) * NX,
        compiler_params=pltpu.CompilerParams(vmem_limit_bytes=20 * MIB),
    )(kept, terms, grads, others, w_key, w_value, key_other, value_other)
    came = [move_x(parts[i], i) for i in (2, 1, 3)]
    return pl.pallas_call(
        final_kernel,
        out_shape=whole((ROWS, 512), BF),
        in_specs=[VM] * 4,
        out_specs=VM,
        compiler_params=pltpu.CompilerParams(vmem_limit_bytes=8 * MIB),
    )(parts[0], *came)


def solution(mesh):
    return jax.shard_map(
        layer,
        mesh=mesh,
        in_specs=(
            P("seq", "tp"),
            P("seq", "tp"),
            P("seq", "tp"),
            P("seq", "tp"),
            P("seq", "tp"),
            P("tp", "seq"),
            P("seq"),
            P(None, "tp"),
            P(None, "tp"),
            P(None, "tp"),
        ),
        out_specs=P("seq", "tp"),
        check_vma=False,
    )
```
